128 devices in a mesh: leaf: 8 (over x, core), front: 16 (over z, y), wave: 1.
Axes of the slice: x: 4, y: 4, z: 4, core: 2. Of those that a mesh axis runs over, the one named last changes fastest.
Arguments:
- sources: float32 [16384, 128], P(('wave', 'front')), may hold values from -48 to 48
- order: int32 [16384], P('front'), may hold values from 0 to 16383, as said below
- diagonal: float32 [16384], P(('wave', 'front')), may hold values from 0.1 to 2
- coupling: float32 [16384, 8192], P(('wave', 'front'), 'leaf'), may hold values from -0.046875 to 0.046875
- interior_inverse: float32 [128, 64, 64], P(('wave', 'leaf')), may hold values from -2 to 6, as said below
- interior_load: float32 [128, 64, 128], P(('wave', 'leaf')), may hold values from -6 to 6
Outputs:
- solution: float32 [16384, 128], P(('wave', 'front'))
- interior_solution: float32 [128, 64, 128], P(('wave', 'leaf'))
The draws below stay inside these ranges and needn't reach their ends.
Inputs may be any that keep to these rules, and one draw needn't show every extreme that they name: `order`: each aligned block of 1024 entries is a permutation of that block's own indices. `interior_inverse`: each matrix is symmetric positive definite.
All inputs are finite; a program needn't handle non-finite values.
Results may differ from the reference program's by a relative error of at most 0.0003.
Values sent between devices are 32-bit elements; how exact they have to be, the bound alone decides.
A program may use at most 64 MiB of HBM per device.

```python
import math
import jax
import jax.numpy as jnp
from jax import lax

SEP_DEV = 1024
NRHS = 128
RANK = 64
ITERS = 4
SEP = 16384
BLOCKS = 128
N_FRONT = 16


def draw_sources(key, part):
    first_key, second_key = jax.random.split(key, 2)
    position = jnp.arange(SEP, dtype=jnp.float32) / SEP
    spread = jax.random.uniform(second_key, (SEP,), jnp.float32, -0.5, 0.5)
    scales = jnp.exp(jnp.log(3.0) * position + jnp.log(10.0) * spread)
    values = jnp.clip(jax.random.normal(first_key, (SEP, NRHS), jnp.float32), -5.0, 5.0)
    return values * scales[:, None]


def draw_order(key, part):
    streams = jax.random.split(key, N_FRONT)
    blocks = jax.vmap(lambda stream: jax.random.permutation(stream, SEP_DEV))(streams)
    offsets = (jnp.arange(N_FRONT, dtype=jnp.int32) * SEP_DEV)[:, None]
    return (blocks.astype(jnp.int32) + offsets).reshape(SEP)


def draw_interior_inverse(key, part):
    first_key, second_key = jax.random.split(key)
    factor = jax.random.normal(first_key, (BLOCKS, RANK, RANK), jnp.float32)
    weights = jax.random.uniform(second_key, (BLOCKS, RANK), jnp.float32, 0.5, 2.0)
    product = jnp.einsum('bij,bkj->bik', factor, factor) * (0.5 / RANK)
    return product + weights[:, :, None] * jnp.eye(RANK, dtype=jnp.float32)


def block_levels(key, dims, pieces, low, high):
    def one(dim, blocks):
        heights = jax.random.uniform(jax.random.fold_in(jax.random.fold_in(key, 6), dim), (blocks,), jnp.float32, low / len(pieces), high / len(pieces))
        return jnp.repeat(jnp.exp(heights), dims[dim] // blocks).reshape((-1,) + (1,) * (len(dims) - dim - 1))

    factor_of = one(*pieces[0])
    for cut in pieces[1:]:
        factor_of = factor_of * one(*cut)
    return factor_of


def scatter_about(key, shape, deviation, bound, cuts=(), kind=jnp.bfloat16):
    result = deviation * jax.random.normal(key, shape, jnp.float32)
    if cuts:
        result = result * block_levels(key, shape, cuts, -0.22, 0.18)
    return jnp.clip(result, -bound, bound).astype(kind)


def setup_inputs(seed: int = 0, part: int = 0) -> dict:
    key_of = jax.random.split(jax.random.key(seed), 7)
    own_keys = jax.random.split(jax.random.fold_in(key_of[6], part), 7)
    sources = draw_sources(jax.random.fold_in(jax.random.fold_in(key_of[6], part), 71), part)
    order = draw_order(jax.random.fold_in(key_of[6], 71), part)
    diagonal = jnp.clip(jnp.exp(math.log(2.0) - 2.9957323 * jax.random.uniform(own_keys[2], (SEP,), jnp.float32) ** block_levels(own_keys[2], (SEP,), ((0, 16),), -0.2, 0.2)), 0.1, 2.0)
    coupling = scatter_about(own_keys[3], (SEP, BLOCKS * RANK), (2 * RANK * BLOCKS) ** -0.5, 0.046875, ((0, 16), (1, 8)), jnp.float32)
    interior_inverse = draw_interior_inverse(jax.random.fold_in(jax.random.fold_in(key_of[6], part), 71), part)
    interior_load = scatter_about(own_keys[5], (BLOCKS, RANK, NRHS), 1.0, 6.0, ((0, 8),), jnp.float32)
    return dict(sources=sources, order=order, diagonal=diagonal, coupling=coupling, interior_inverse=interior_inverse, interior_load=interior_load)


HIGHEST = lax.Precision.HIGHEST


def reference(sources, order, diagonal, coupling, interior_inverse, interior_load):
    loads = jnp.take(sources, order.astype(jnp.int32), axis=0)

    def condense(projected):
        shaped = projected.reshape(BLOCKS, RANK, NRHS)
        return jnp.einsum("bij,bjn->bin", interior_inverse, shaped, precision=HIGHEST)

    def operate(direction):
        projected = jnp.einsum("sk,sn->kn", coupling, direction, precision=HIGHEST)
        coeffs = condense(projected).reshape(BLOCKS * RANK, NRHS)
        return diagonal[:, None] * direction + jnp.einsum("sk,kn->sn", coupling, coeffs, precision=HIGHEST)

    solution = jnp.zeros_like(loads)
    residual = loads
    direction = loads
    norm_now = jnp.sum(residual * residual, axis=0)
    for iteration in range(ITERS):
        image = operate(direction)
        step_size = norm_now / jnp.sum(direction * image, axis=0)
        solution = solution + step_size * direction
        residual = residual - step_size * image
        norm_next = jnp.sum(residual * residual, axis=0)
        direction = residual + (norm_next / norm_now) * direction
        norm_now = norm_next
    projected = jnp.einsum("sk,sn->kn", coupling, solution, precision=HIGHEST).reshape(BLOCKS, RANK, NRHS)
    interior_solution = jnp.einsum("bij,bjn->bin", interior_inverse, interior_load - projected, precision=HIGHEST)
    return (solution, interior_solution)
```

```python
import functools

import jax
import jax.numpy as jnp
from jax import lax
from jax.experimental import pallas as pl
from jax.experimental.pallas import tpu as pltpu
from jax.sharding import PartitionSpec as P

ITERS = 4
NZ, NY, NX, CORES = 4, 4, 4, 2
EXTRA = 8
HIGHEST = lax.Precision.HIGHEST
F32 = jnp.float32
BF16 = jnp.bfloat16


def far_first(n):
    return sorted(range(n), key=lambda d: -min(d, n - d))


def split(value):
    high = value.astype(BF16)
    return high, (value - high.astype(F32)).astype(BF16)


def front_solve(
    grid,
    order_ref,
    sources_ref,
    diag_ref,
    coupling_hbm,
    inverse_ref,
    load_ref,
    x_ref,
    interior_ref,
    stage,
    c_high,
    c_low,
    t_high,
    t_low,
    rhs,
    image,
    residual,
    direction,
    diag_full,
    w_send,
    w_recv,
    c_send,
    c_full,
    half_send,
    half_recv,
    share,
    share_recv,
    merged,
    tr_ref,
    td_ref,
    rr_ref,
    q_send,
    q_recv,
    stage_sem,
    w_ssem,
    w_rsem,
    c_ssem,
    c_rsem,
    h_ssem,
    h_rsem,
    s_ssem,
    s_rsem,
    m_ssem,
    m_rsem,
    p_ssem,
    p_rsem,
    q_ssem,
    q_rsem,
):
    nz, ny, nx = grid
    fronts, leaves = nz * ny, nx * CORES
    rows, cols = image.shape
    rank = inverse_ref.shape[1]
    half = rows // 2
    piece = half // nx
    front = lax.axis_index("front")
    leaf = lax.axis_index("leaf")
    z, y = front // ny, front % ny
    x, core = leaf // CORES, leaf % CORES

    z_steps, y_steps, x_steps = far_first(nz), far_first(ny), far_first(nx)
    peers = [(dz, dy) for dz in z_steps for dy in y_steps if dz or dy]

    def front_at(dz, dy):
        return ((z + dz) % nz) * ny + (y + dy) % ny

    def leaf_at(dx):
        return ((x + dx) % nx) * CORES + core

    partner = x * CORES + (1 - core)

    stages = []
    step_rows = rows // stage_sem.shape[0]
    for i in range(stage_sem.shape[0]):
        part = pl.ds(i * step_rows, step_rows)
        stages.append(
            pltpu.make_async_copy(coupling_hbm.at[part], stage.at[part], stage_sem.at[i])
        )
        stages[-1].start()

    barrier = pltpu.get_barrier_semaphore()
    for dz, dy in peers:
        pl.semaphore_signal(barrier, inc=1, device_id={"front": front_at(dz, dy)})
    for d in range(1, leaves):
        pl.semaphore_signal(barrier, inc=1, device_id={"leaf": (leaf + d) % leaves})

    def take(i, _):
        for j in range(8):
            at = i * 8 + j
            image[pl.ds(at, 1), :] = sources_ref[pl.ds(lax.rem(order_ref[at], rows), 1), :]
        return 0

    lax.fori_loop(0, rows // 8, take, 0)

    tile = 128
    for i in range(rows // tile):
        diag_full[i * tile : (i + 1) * tile, :] = jnp.broadcast_to(
            diag_ref[i : i + 1, :], (tile, tile)
        ).T
    zero = jnp.zeros((rows, cols), F32)
    x_ref[...] = zero
    residual[...] = zero
    direction[...] = zero
    tr_ref[...] = jnp.zeros_like(tr_ref)
    td_ref[...] = jnp.zeros_like(td_ref)
    rr_ref[...] = jnp.zeros_like(rr_ref)

    for i, copy in enumerate(stages):
        copy.wait()
        for r in range(i * step_rows, (i + 1) * step_rows, tile):

            def turn(j, _, r=r):
                at = pl.ds(pl.multiple_of(j * tile, tile), tile)
                block = stage[r : r + tile, at]
                high, low = split(block)
                c_high[r : r + tile, at] = high
                c_low[r : r + tile, at] = low
                high, low = split(block.T)
                t_high[at, r : r + tile] = high
                t_low[at, r : r + tile] = low
                return 0

            lax.fori_loop(0, stage.shape[1] // tile, turn, 0)

    def split_rows(i, block):
        high, low = split(block)
        rhs[i : i + tile, 0:cols] = high
        rhs[i : i + tile, cols : 2 * cols] = low

    for i in range(0, rows, tile):
        split_rows(i, image[i : i + tile, :])

    pl.semaphore_wait(barrier, len(peers) + leaves - 1)

    def times(high_ref, low_ref, at):
        both = jnp.dot(high_ref[at, :], rhs[...], preferred_element_type=F32)
        both += jnp.dot(low_ref[at, :], rhs[...], preferred_element_type=F32)
        return both[:, :cols] + both[:, cols:]

    def project(k, is_first, last):
        sums = [jnp.zeros((8, cols), F32)] * 3
        for i in range(0, rows, tile):
            im = image[i : i + tile, :]
            for n, other in enumerate(
                (direction[i : i + tile, :], residual[i : i + tile, :], im)
            ):
                sums[n] = sums[n] + (other * im).reshape(-1, 8, cols).sum(axis=0)
        dots = jnp.concatenate(
            [s.sum(axis=0, keepdims=True) for s in sums] + [jnp.zeros((EXTRA - 3, cols), F32)]
        )
        pending = []
        for dz in z_steps:
            at_z = (z + dz) % nz
            span = ny * rank
            at = pl.ds(pl.multiple_of(at_z * span, span), span)
            out = times(t_high, t_low, at)
            for j in range(ny):
                w_send[at_z * ny + j, 0:rank, :] = out[j * rank : (j + 1) * rank]
                w_send[at_z * ny + j, rank:, :] = dots
            for dy in y_steps:
                if dz or dy:
                    to = front_at(dz, dy)
                    n = dz * ny + dy
                    copy = pltpu.make_async_remote_copy(
                        src_ref=w_send.at[to],
                        dst_ref=w_recv.at[front],
                        send_sem=w_ssem.at[n],
                        recv_sem=w_rsem.at[n],
                        device_id={"front": to},
                    )
                    copy.start()
                    pending.append(copy)
        w_recv[front] = w_send[front]
        for copy in pending:
            copy.wait_recv()
        total = w_recv[0]
        for n in range(1, fronts):
            total = total + w_recv[n]
        w = total[0:rank]
        curvature, cross, square = (total[rank + n : rank + n + 1] for n in range(3))
        rr = rr_ref[...]
        alpha = jnp.where(is_first, -1.0, rr / curvature)
        rr_next = rr - 2.0 * alpha * cross + alpha * alpha * square
        beta = jnp.where(is_first, 0.0, rr_next / rr)
        rr_ref[...] = rr_next
        tr = tr_ref[...] - alpha * w
        td = tr + beta * td_ref[...]
        tr_ref[...] = tr
        td_ref[...] = td
        coeff = jnp.dot(inverse_ref[front], td, precision=HIGHEST, preferred_element_type=F32)

        def advance():
            q = jnp.zeros((8, cols), F32)
            for i in range(0, rows, tile):
                at = slice(i, i + tile)
                x_ref[at, :] += alpha * direction[at, :]
                res = residual[at, :] - alpha * image[at, :]
                residual[at, :] = res
                new = res + beta * direction[at, :]
                direction[at, :] = new
                if last:
                    q = q + (diag_full[at, :] * new * new).reshape(-1, 8, cols).sum(axis=0)
            return q

        c_send[0:rank, :] = coeff
        c_full[k, front, 0:rank, :] = coeff
        if last:
            q = advance() * (1.0 / leaves)
            q = q + (td * coeff).reshape(-1, 8, cols).sum(axis=0)
            c_send[rank:, :] = q
            c_full[k, front, rank:, :] = q
        size = rank + (8 if last else 0)
        spread = []
        for dz, dy in peers:
            n = dz * ny + dy
            copy = pltpu.make_async_remote_copy(
                src_ref=c_send.at[0:size],
                dst_ref=c_full.at[k, front, 0:size],
                send_sem=c_ssem.at[n],
                recv_sem=c_rsem.at[n],
                device_id={"front": front_at(dz, dy)},
            )
            copy.start()
            spread.append(copy)
        if not last:
            advance()
        for copy in pending:
            copy.wait_send()
        return alpha, spread

    def subtract(k, step):
        for n in range(fronts):
            interior_ref[n] = interior_ref[n] - step * c_full[k, n, 0:rank, :]

    def iterate(k, _):
        is_first = k == 0
        alpha, spread = project(k, is_first, False)

        @pl.when(is_first)
        def _():
            for n in range(fronts):
                interior_ref[n] = jnp.dot(
                    inverse_ref[n], load_ref[n], precision=HIGHEST, preferred_element_type=F32
                )

        @pl.when(k > 0)
        def _():
            subtract(k - 1, alpha)

        for copy in spread:
            copy.wait_recv()
        for n in range(fronts):
            high, low = split(c_full[k, n, 0:rank, :])
            rhs[n * rank : (n + 1) * rank, 0:cols] = high
            rhs[n * rank : (n + 1) * rank, cols : 2 * cols] = low

        theirs = pl.multiple_of((1 - core) * half, half)
        mine = pl.multiple_of(core * half, half)
        for i in range(0, half, tile * 2):
            n = min(tile * 2, half)
            half_send[i : i + n, :] = times(c_high, c_low, pl.ds(theirs + i, n))
        over = pltpu.make_async_remote_copy(
            src_ref=half_send,
            dst_ref=half_recv,
            send_sem=h_ssem,
            recv_sem=h_rsem,
            device_id={"leaf": partner},
        )
        over.start()
        for i in range(0, half, tile * 2):
            n = min(tile * 2, half)
            out = times(c_high, c_low, pl.ds(mine + i, n))
            for j in range(0, n, piece):
                share[(i + j) // piece] = out[j : j + piece]
        for copy in spread:
            copy.wait_send()
        over.wait_recv()
        for n in range(nx):
            share[n] = share[n] + half_recv[n * piece : (n + 1) * piece, :]
        moves = []
        for dx in x_steps:
            if dx:
                copy = pltpu.make_async_remote_copy(
                    src_ref=share.at[(x + dx) % nx],
                    dst_ref=share_recv.at[x],
                    send_sem=s_ssem.at[dx],
                    recv_sem=s_rsem.at[dx],
                    device_id={"leaf": leaf_at(dx)},
                )
                copy.start()
                moves.append(copy)
        share_recv[x] = share[x]
        for copy in moves:
            copy.wait_recv()
        total = share_recv[0]
        for n in range(1, nx):
            total = total + share_recv[n]
        own = core * nx + x
        merged[own] = total
        out_x = []
        for dx in x_steps:
            if dx:
                copy = pltpu.make_async_remote_copy(
                    src_ref=merged.at[own],
                    dst_ref=merged.at[own],
                    send_sem=m_ssem.at[dx],
                    recv_sem=m_rsem.at[dx],
                    device_id={"leaf": leaf_at(dx)},
                )
                copy.start()
                out_x.append((dx, copy))

        def pass_on(dx):
            at = core * nx + (x - dx + nx) % nx
            copy = pltpu.make_async_remote_copy(
                src_ref=merged.at[at],
                dst_ref=merged.at[at],
                send_sem=p_ssem.at[dx],
                recv_sem=p_rsem.at[dx],
                device_id={"leaf": partner},
            )
            copy.start()
            return copy

        passed = [pass_on(0)]
        for copy in moves:
            copy.wait_send()
        over.wait_send()
        for dx, copy in reversed(out_x):
            copy.wait_recv()
            passed.append(pass_on(dx))
        for copy in passed:
            copy.wait_recv()
        for n in range(rows // piece):
            at = slice(n * piece, (n + 1) * piece)
            new = diag_full[at, :] * direction[at, :] + merged[n]
            image[at, :] = new
            high, low = split(new)
            rhs[at, 0:cols] = high
            rhs[at, cols : 2 * cols] = low
        for dx, copy in out_x:
            copy.wait_send()
        for copy in passed:
            copy.wait_send()
        return 0

    lax.fori_loop(0, ITERS - 1, iterate, 0)

    end = ITERS - 1
    alpha, spread = project(end, False, True)
    subtract(end - 1, alpha)
    for copy in spread:
        copy.wait_recv()
    q = c_full[end, 0, rank:, :]
    for n in range(1, fronts):
        q = q + c_full[end, n, rank:, :]
    q_send[...] = q
    q_recv[leaf] = q
    last_sums = []
    for d in range(1, leaves):
        copy = pltpu.make_async_remote_copy(
            src_ref=q_send,
            dst_ref=q_recv.at[leaf],
            send_sem=q_ssem.at[d],
            recv_sem=q_rsem.at[d],
            device_id={"leaf": (leaf + d) % leaves},
        )
        copy.start()
        last_sums.append(copy)
    for copy in spread:
        copy.wait_send()
    for copy in last_sums:
        copy.wait_recv()
    q = q_recv[0]
    for n in range(1, leaves):
        q = q + q_recv[n]
    step = rr_ref[...] / q.sum(axis=0, keepdims=True)
    for i in range(0, rows, tile):
        at = slice(i, i + tile)
        x_ref[at, :] += step * direction[at, :]
    subtract(end, step)
    for copy in last_sums:
        copy.wait_send()


def per_device(sources, order, diagonal, coupling, interior_inverse, interior_load, grid=(NZ, NY, NX)):
    nz, ny, nx = grid
    fronts, leaves = nz * ny, nx * CORES
    rows, cols = sources.shape
    depth = coupling.shape[1]
    blocks, rank = interior_inverse.shape[:2]
    assert blocks == fronts and depth == blocks * rank
    piece = rows // 2 // nx
    vmem = pl.BlockSpec(memory_space=pltpu.VMEM)
    dma = pltpu.SemaphoreType.DMA
    field = pltpu.VMEM((rows, cols), F32)
    return tuple(
        pl.pallas_call(
            functools.partial(front_solve, grid),
            out_shape=(
                jax.ShapeDtypeStruct((rows, cols), F32),
                jax.ShapeDtypeStruct(interior_load.shape, F32),
            ),
            in_specs=[
                pl.BlockSpec(memory_space=pltpu.SMEM),
                vmem,
                vmem,
                pl.BlockSpec(memory_space=pl.ANY),
                vmem,
                vmem,
            ],
            out_specs=(vmem, vmem),
            scratch_shapes=[
                pltpu.VMEM((rows, depth), F32),
                pltpu.VMEM((rows, depth), BF16),
                pltpu.VMEM((rows, depth), BF16),
                pltpu.VMEM((depth, rows), BF16),
                pltpu.VMEM((depth, rows), BF16),
                pltpu.VMEM((max(rows, depth), 2 * cols), BF16),
                field,
                field,
                field,
                field,
                pltpu.VMEM((fronts, rank + EXTRA, cols), F32),
                pltpu.VMEM((fronts, rank + EXTRA, cols), F32),
                pltpu.VMEM((rank + EXTRA, cols), F32),
                pltpu.VMEM((ITERS, fronts, rank + EXTRA, cols), F32),
                pltpu.VMEM((rows // 2, cols), F32),
                pltpu.VMEM((rows // 2, cols), F32),
                pltpu.VMEM((nx, piece, cols), F32),
                pltpu.VMEM((nx, piece, cols), F32),
                pltpu.VMEM((CORES * nx, piece, cols), F32),
                pltpu.VMEM((rank, cols), F32),
                pltpu.VMEM((rank, cols), F32),
                pltpu.VMEM((1, cols), F32),
                pltpu.VMEM((8, cols), F32),
                pltpu.VMEM((leaves, 8, cols), F32),
                dma((min(4, rows // 128),)),
                dma((fronts,)),
                dma((fronts,)),
                dma((fronts,)),
                dma((fronts,)),
                dma,
                dma,
                dma((nx,)),
                dma((nx,)),
                dma((nx,)),
                dma((nx,)),
                dma((nx,)),
                dma((nx,)),
                dma((leaves,)),
                dma((leaves,)),
            ],
            compiler_params=pltpu.CompilerParams(
                collective_id=0, has_side_effects=True, vmem_limit_bytes=48 << 20
            ),
            name="front_solve",
        )(
            order,
            sources,
            diagonal.reshape(rows // 128, 128),
            coupling,
            interior_inverse,
            interior_load,
        )
    )


def solution(mesh):
    in_specs = (
        P(("wave", "front"), None),
        P("front"),
        P(("wave", "front")),
        P(("wave", "front"), "leaf"),
        P(("wave", "leaf"), None, None),
        P(("wave", "leaf"), None, None),
    )
    out_specs = (P(("wave", "front"), None), P(("wave", "leaf"), None, None))
    return jax.shard_map(
        per_device, mesh=mesh, in_specs=in_specs, out_specs=out_specs, check_vma=False
    )
```

```python
import functools

import jax
import jax.numpy as jnp
from jax import lax
from jax.experimental import pallas as pl
from jax.experimental.pallas import tpu as pltpu
from jax.sharding import PartitionSpec as P

ITERS = 4
NZ, NY, NX, CORES = 4, 4, 4, 2
EXTRA = 8
SUMS = 3
HIGHEST = lax.Precision.HIGHEST
F32 = jnp.float32
BF16 = jnp.bfloat16


def far_first(n):
    return sorted(range(n), key=lambda d: -min(d, n - d))


def split(value):
    high = value.astype(BF16)
    return high, (value - high.astype(F32)).astype(BF16)


def front_solve(
    grid,
    order_hbm,
    sources_hbm,
    diag_hbm,
    coupling_hbm,
    inverse_hbm,
    load_hbm,
    x_ref,
    direction,
    interior_ref,
    last_ref,
    step_ref,
    order_ref,
    sources_ref,
    diag_ref,
    inverse_ref,
    load_ref,
    stage,
    c_high,
    c_low,
    t_high,
    t_low,
    rhs,
    turned,
    image,
    residual,
    diag_full,
    w_send,
    w_recv,
    c_send,
    c_full,
    half_send,
    half_recv,
    share,
    share_recv,
    merged,
    tr_ref,
    td_ref,
    rr_ref,
    q_send,
    q_recv,
    g_send,
    g_recv,
    load_sem,
    stage_sem,
    w_ssem,
    w_rsem,
    c_ssem,
    c_rsem,
    h_ssem,
    h_rsem,
    s_ssem,
    s_rsem,
    m_ssem,
    m_rsem,
    p_ssem,
    p_rsem,
    q_ssem,
    q_rsem,
    g_ssem,
    g_rsem,
):
    nz, ny, nx = grid
    fronts, leaves = nz * ny, nx * CORES
    rows, cols = image.shape
    rank = inverse_ref.shape[1]
    half = rows // 2
    piece = half // nx
    front = lax.axis_index("front")
    leaf = lax.axis_index("leaf")
    z, y = front // ny, front % ny
    x, core = leaf // CORES, leaf % CORES

    z_steps, y_steps, x_steps = far_first(nz), far_first(ny), far_first(nx)
    peers = [(dz, dy) for dz in z_steps for dy in y_steps if dz or dy]

    def front_at(dz, dy):
        return ((z + dz) % nz) * ny + (y + dy) % ny

    def leaf_at(dx):
        return ((x + dx) % nx) * CORES + core

    partner = x * CORES + (1 - core)

    loads = [
        pltpu.make_async_copy(source, here, load_sem.at[i])
        for i, (source, here) in enumerate(
            (
                (order_hbm, order_ref),
                (sources_hbm, sources_ref),
                (diag_hbm, diag_ref),
                (inverse_hbm, inverse_ref),
                (load_hbm, load_ref),
            )
        )
    ]
    for copy in loads[:2]:
        copy.start()
    stages = []
    step_rows = rows // stage_sem.shape[0]
    for i in range(stage_sem.shape[0]):
        part = pl.ds(i * step_rows, step_rows)
        stages.append(
            pltpu.make_async_copy(coupling_hbm.at[part], stage.at[part], stage_sem.at[i])
        )
        stages[-1].start()
    for copy in loads[2:]:
        copy.start()

    barrier = pltpu.get_barrier_semaphore()
    for dz, dy in peers:
        pl.semaphore_signal(barrier, inc=1, device_id={"front": front_at(dz, dy)})
    for d in range(1, leaves):
        pl.semaphore_signal(barrier, inc=1, device_id={"leaf": (leaf + d) % leaves})

    tile = 128
    for copy in loads[:2]:
        copy.wait()

    def take(i, _):
        for j in range(16):
            at = i * 16 + j
            image[pl.ds(at, 1), :] = sources_ref[pl.ds(order_ref[at] & (rows - 1), 1), :]
        return 0

    lax.fori_loop(0, rows // 16, take, 0)
    for i in range(0, rows, tile):
        high, low = split(image[i : i + tile, :].T)
        turned[0:cols, i : i + tile] = high
        turned[cols:, i : i + tile] = low
    x_ref[...] = jnp.zeros((rows, cols), F32)

    for i, copy in enumerate(stages):
        copy.wait()

        def divide(j, _, i=i):
            at = pl.ds(pl.multiple_of(i * step_rows + j * 16, 16), 16)
            high, low = split(stage[at, :])
            c_high[at, :] = high
            c_low[at, :] = low
            return 0

        lax.fori_loop(0, step_rows // 16, divide, 0)

    def turn(start, stop):
        def columns(j, _):
            for r in range(start, stop, tile):
                at = pl.ds(pl.multiple_of(j * tile, tile), tile)
                high, low = split(stage[r : r + tile, at].T)
                t_high[at, r : r + tile] = high
                t_low[at, r : r + tile] = low
            return 0

        lax.fori_loop(0, stage.shape[1] // tile, columns, 0)

    def spread_diagonal():
        for i in range(rows // tile):
            diag_full[i * tile : (i + 1) * tile, :] = jnp.broadcast_to(
                diag_ref[i : i + 1, :], (tile, tile)
            ).T

    def start_interior():
        for n in range(fronts):
            interior_ref[n * rank : (n + 1) * rank, :] = jnp.dot(
                inverse_ref[n], load_ref[n], precision=HIGHEST, preferred_element_type=F32
            )

    pl.semaphore_wait(barrier, len(peers) + leaves - 1)

    def times(high_ref, low_ref, at):
        both = jnp.dot(high_ref[at, :], rhs[...], preferred_element_type=F32)
        both += jnp.dot(low_ref[at, :], rhs[...], preferred_element_type=F32)
        return both[:, :cols] + both[:, cols:]

    def times_turned(at):
        both = jnp.dot(turned[...], c_high[:, at], preferred_element_type=F32)
        both += jnp.dot(turned[...], c_low[:, at], preferred_element_type=F32)
        both = both[:cols] + both[cols:]
        n = both.shape[1]
        return jnp.concatenate([both[:, i : i + tile].T for i in range(0, n, tile)])

    def project(k, is_first, last):
        sums = [jnp.zeros((8, cols), F32)] * SUMS
        for i in range(0, rows, tile):
            im = image[i : i + tile, :]
            others = (im, im, im) if is_first else (direction[i : i + tile, :], residual[i : i + tile, :], im)
            for n, other in enumerate(others):
                sums[n] = sums[n] + (other * im).reshape(-1, 8, cols).sum(axis=0)
        dots = jnp.concatenate(
            [s.sum(axis=0, keepdims=True) for s in sums] + [jnp.zeros((EXTRA - SUMS, cols), F32)]
        )
        pending = []
        for dz in z_steps:
            at_z = (z + dz) % nz
            span = ny * rank
            at = pl.ds(pl.multiple_of(at_z * span, span), span)
            out = times_turned(at) if is_first else times(t_high, t_low, at)
            for j in range(ny):
                w_send[at_z * ny + j, 0:rank, :] = out[j * rank : (j + 1) * rank]
                w_send[at_z * ny + j, rank:, :] = dots
            for dy in y_steps:
                if dz or dy:
                    to = front_at(dz, dy)
                    n = dz * ny + dy
                    copy = pltpu.make_async_remote_copy(
                        src_ref=w_send.at[to, 0 : rank + SUMS],
                        dst_ref=w_recv.at[front, 0 : rank + SUMS],
                        send_sem=w_ssem.at[n],
                        recv_sem=w_rsem.at[n],
                        device_id={"front": to},
                    )
                    copy.start()
                    pending.append(copy)
        w_recv[front, 0 : rank + SUMS, :] = w_send[front, 0 : rank + SUMS, :]
        if is_first:
            turn(0, rows // 2)
            loads[3].wait()
        for copy in pending:
            copy.wait_recv()
        w = w_recv[0, 0:rank, :]
        curvature, cross, square = (w_recv[0, rank + n : rank + n + 1, :] for n in range(SUMS))
        for n in range(1, fronts):
            w = w + w_recv[n, 0:rank, :]
            curvature = curvature + w_recv[n, rank : rank + 1, :]
            cross = cross + w_recv[n, rank + 1 : rank + 2, :]
            square = square + w_recv[n, rank + 2 : rank + 3, :]
        if is_first:
            alpha = beta = None
            rr_ref[...] = square
            tr = td = w
        else:
            rr = rr_ref[...]
            alpha = rr / curvature
            rr_next = rr - 2.0 * alpha * cross + alpha * alpha * square
            beta = rr_next / rr
            rr_ref[...] = rr_next
            tr = tr_ref[...] - alpha * w
            td = tr + beta * td_ref[...]
        tr_ref[...] = tr
        td_ref[...] = td
        coeff = jnp.dot(inverse_ref[front], td, precision=HIGHEST, preferred_element_type=F32)

        here = c_full.at[k] if not last else last_ref
        rows_here = pl.ds(pl.multiple_of(front * rank, rank), rank)
        c_send[...] = coeff
        here[rows_here, :] = coeff
        spread = []
        for dz, dy in peers:
            n = dz * ny + dy
            copy = pltpu.make_async_remote_copy(
                src_ref=c_send,
                dst_ref=here.at[rows_here],
                send_sem=c_ssem.at[n],
                recv_sem=c_rsem.at[n],
                device_id={"front": front_at(dz, dy)},
            )
            copy.start()
            spread.append(copy)
        own = (td * coeff).reshape(-1, 8, cols).sum(axis=0) if last else None
        return alpha, beta, own, spread, pending

    def advance(alpha, beta):
        for i in range(0, rows, tile):
            at = slice(i, i + tile)
            x_ref[at, :] += alpha * direction[at, :]
            res = residual[at, :] - alpha * image[at, :]
            residual[at, :] = res
            direction[at, :] = res + beta * direction[at, :]

    def subtract(k, step):
        for i in range(0, fronts * rank, tile):
            at = slice(i, i + tile)
            interior_ref[at, :] = interior_ref[at, :] - step * c_full[k, at, :]

    def iterate(k, is_first):
        alpha, beta, _, spread, pending = project(k, is_first, False)
        if is_first:
            residual[...] = image[...]
            direction[...] = image[...]
            for copy in (loads[2], loads[4]):
                copy.wait()
            turn(rows // 2, rows)
            spread_diagonal()
            start_interior()
        else:
            advance(alpha, beta)
            subtract(k - 1, alpha)
        for copy in pending:
            copy.wait_send()

        for copy in spread:
            copy.wait_recv()
        for i in range(0, fronts * rank, tile):
            high, low = split(c_full[k, i : i + tile, :])
            rhs[i : i + tile, 0:cols] = high
            rhs[i : i + tile, cols : 2 * cols] = low

        theirs = pl.multiple_of((1 - core) * half, half)
        mine = pl.multiple_of(core * half, half)
        for i in range(0, half, tile * 2):
            n = min(tile * 2, half)
            half_send[i : i + n, :] = times(c_high, c_low, pl.ds(theirs + i, n))
        over = pltpu.make_async_remote_copy(
            src_ref=half_send,
            dst_ref=half_recv,
            send_sem=h_ssem,
            recv_sem=h_rsem,
            device_id={"leaf": partner},
        )
        over.start()
        for i in range(0, half, tile * 2):
            n = min(tile * 2, half)
            out = times(c_high, c_low, pl.ds(mine + i, n))
            for j in range(0, n, piece):
                share[(i + j) // piece] = out[j : j + piece]
        for copy in spread:
            copy.wait_send()
        over.wait_recv()
        for n in range(nx):
            share[n] = share[n] + half_recv[n * piece : (n + 1) * piece, :]
        moves = []
        for dx in x_steps:
            if dx:
                copy = pltpu.make_async_remote_copy(
                    src_ref=share.at[(x + dx) % nx],
                    dst_ref=share_recv.at[x],
                    send_sem=s_ssem.at[dx],
                    recv_sem=s_rsem.at[dx],
                    device_id={"leaf": leaf_at(dx)},
                )
                copy.start()
                moves.append(copy)
        share_recv[x] = share[x]
        for copy in moves:
            copy.wait_recv()
        total = share_recv[0]
        for n in range(1, nx):
            total = total + share_recv[n]
        own = core * nx + x
        merged[own] = total
        out_x = []
        for dx in x_steps:
            if dx:
                copy = pltpu.make_async_remote_copy(
                    src_ref=merged.at[own],
                    dst_ref=merged.at[own],
                    send_sem=m_ssem.at[dx],
                    recv_sem=m_rsem.at[dx],
                    device_id={"leaf": leaf_at(dx)},
                )
                copy.start()
                out_x.append((dx, copy))

        def pass_on(dx):
            at = core * nx + (x - dx + nx) % nx
            copy = pltpu.make_async_remote_copy(
                src_ref=merged.at[at],
                dst_ref=merged.at[at],
                send_sem=p_ssem.at[dx],
                recv_sem=p_rsem.at[dx],
                device_id={"leaf": partner},
            )
            copy.start()
            return copy

        passed = [pass_on(0)]
        for copy in moves:
            copy.wait_send()
        over.wait_send()
        for dx, copy in reversed(out_x):
            copy.wait_recv()
            passed.append(pass_on(dx))
        for copy in passed:
            copy.wait_recv()
        for n in range(rows // piece):
            at = slice(n * piece, (n + 1) * piece)
            new = diag_full[at, :] * direction[at, :] + merged[n]
            image[at, :] = new
            high, low = split(new)
            rhs[at, 0:cols] = high
            rhs[at, cols : 2 * cols] = low
        for dx, copy in out_x:
            copy.wait_send()
        for copy in passed:
            copy.wait_send()
        return 0

    iterate(0, True)
    lax.fori_loop(1, ITERS - 1, lambda k, _: iterate(k, False), 0)

    end = ITERS - 1
    alpha, beta, own, spread, pending = project(end, False, True)
    q_send[...] = own
    q_recv[leaf] = own
    over_leaf = []
    for d in range(1, leaves):
        copy = pltpu.make_async_remote_copy(
            src_ref=q_send,
            dst_ref=q_recv.at[leaf],
            send_sem=q_ssem.at[d],
            recv_sem=q_rsem.at[d],
            device_id={"leaf": (leaf + d) % leaves},
        )
        copy.start()
        over_leaf.append(copy)
    advance(alpha, beta)
    q = jnp.zeros((8, cols), F32)
    for i in range(0, rows, tile):
        new = direction[i : i + tile, :]
        q = q + (diag_full[i : i + tile, :] * new * new).reshape(-1, 8, cols).sum(axis=0)
    for copy in over_leaf:
        copy.wait_recv()
    for n in range(leaves):
        q = q + q_recv[n]
    g_send[...] = q
    g_recv[front] = q
    over_front = []
    for dz, dy in peers:
        n = dz * ny + dy
        copy = pltpu.make_async_remote_copy(
            src_ref=g_send,
            dst_ref=g_recv.at[front],
            send_sem=g_ssem.at[n],
            recv_sem=g_rsem.at[n],
            device_id={"front": front_at(dz, dy)},
        )
        copy.start()
        over_front.append(copy)
    subtract(end - 1, alpha)
    for copy in pending + over_leaf:
        copy.wait_send()
    for copy in spread + over_front:
        copy.wait_recv()
    q = g_recv[0]
    for n in range(1, fronts):
        q = q + g_recv[n]
    step_ref[...] = rr_ref[...] / q.sum(axis=0, keepdims=True)
    for copy in spread + over_front:
        copy.wait_send()


def per_device(sources, order, diagonal, coupling, interior_inverse, interior_load, grid=(NZ, NY, NX)):
    nz, ny, nx = grid
    fronts, leaves = nz * ny, nx * CORES
    rows, cols = sources.shape
    depth = coupling.shape[1]
    blocks, rank = interior_inverse.shape[:2]
    assert blocks == fronts and depth == blocks * rank
    piece = rows // 2 // nx
    vmem = pl.BlockSpec(memory_space=pltpu.VMEM)
    dma = pltpu.SemaphoreType.DMA
    field = pltpu.VMEM((rows, cols), F32)
    hbm = pl.BlockSpec(memory_space=pltpu.HBM)
    whole = jax.ShapeDtypeStruct((rows, cols), F32)
    inner = jax.ShapeDtypeStruct((depth, cols), F32)
    x, direction, interior, coeff, step = pl.pallas_call(
        functools.partial(front_solve, grid),
        out_shape=(whole, whole, inner, inner, jax.ShapeDtypeStruct((1, cols), F32)),
        in_specs=[hbm] * 6,
        out_specs=(vmem,) * 5,
        scratch_shapes=[
            pltpu.SMEM((rows,), jnp.int32),
            field,
            pltpu.VMEM((rows // 128, 128), F32),
            pltpu.VMEM(interior_inverse.shape, F32),
            pltpu.VMEM(interior_load.shape, F32),
            pltpu.VMEM((rows, depth), F32),
            pltpu.VMEM((rows, depth), BF16),
            pltpu.VMEM((rows, depth), BF16),
            pltpu.VMEM((depth, rows), BF16),
            pltpu.VMEM((depth, rows), BF16),
            pltpu.VMEM((max(rows, depth), 2 * cols), BF16),
            pltpu.VMEM((2 * cols, rows), BF16),
            field,
            field,
            field,
            pltpu.VMEM((fronts, rank + EXTRA, cols), F32),
            pltpu.VMEM((fronts, rank + EXTRA, cols), F32),
            pltpu.VMEM((rank, cols), F32),
            pltpu.VMEM((ITERS - 1, depth, cols), F32),
            pltpu.VMEM((rows // 2, cols), F32),
            pltpu.VMEM((rows // 2, cols), F32),
            pltpu.VMEM((nx, piece, cols), F32),
            pltpu.VMEM((nx, piece, cols), F32),
            pltpu.VMEM((CORES * nx, piece, cols), F32),
            pltpu.VMEM((rank, cols), F32),
            pltpu.VMEM((rank, cols), F32),
            pltpu.VMEM((1, cols), F32),
            pltpu.VMEM((8, cols), F32),
            pltpu.VMEM((leaves, 8, cols), F32),
            pltpu.VMEM((8, cols), F32),
            pltpu.VMEM((fronts, 8, cols), F32),
            dma((5,)),
            dma((min(8, rows // 128),)),
            dma((fronts,)),
            dma((fronts,)),
            dma((fronts,)),
            dma((fronts,)),
            dma,
            dma,
            dma((nx,)),
            dma((nx,)),
            dma((nx,)),
            dma((nx,)),
            dma((nx,)),
            dma((nx,)),
            dma((leaves,)),
            dma((leaves,)),
            dma((fronts,)),
            dma((fronts,)),
        ],
        compiler_params=pltpu.CompilerParams(
            collective_id=0, has_side_effects=True, vmem_limit_bytes=48 << 20
        ),
        name="front_solve",
    )(
        *(
            pltpu.with_memory_space_constraint(value, pltpu.HBM)
            for value in (
                order,
                sources,
                diagonal.reshape(rows // 128, 128),
                coupling,
                interior_inverse,
                interior_load,
            )
        )
    )
    interior = interior - step * coeff
    return x + step * direction, interior.reshape(interior_load.shape)


def solution(mesh):
    in_specs = (
        P(("wave", "front"), None),
        P("front"),
        P(("wave", "front")),
        P(("wave", "front"), "leaf"),
        P(("wave", "leaf"), None, None),
        P(("wave", "leaf"), None, None),
    )
    out_specs = (P(("wave", "front"), None), P(("wave", "leaf"), None, None))
    return jax.shard_map(
        per_device, mesh=mesh, in_specs=in_specs, out_specs=out_specs, check_vma=False
    )
```

```python
import functools

import jax
import jax.numpy as jnp
from jax import lax
from jax.experimental import pallas as pl
from jax.experimental.pallas import tpu as pltpu
from jax.sharding import PartitionSpec as P

ITERS = 4
NZ, NY, NX, CORES = 4, 4, 4, 2
EXTRA = 8
SUMS = 3
STREAMS = 2
HIGHEST = lax.Precision.HIGHEST
F32 = jnp.float32
BF16 = jnp.bfloat16


def far_first(n):
    return sorted(range(n), key=lambda d: -min(d, n - d))


def split(value):
    high = value.astype(BF16)
    return high, (value - high.astype(F32)).astype(BF16)


def front_solve(
    grid,
    order_hbm,
    sources_hbm,
    diag_hbm,
    coupling_hbm,
    inverse_hbm,
    load_hbm,
    x_out,
    direction_out,
    interior_out,
    last_out,
    step_ref,
    order_ref,
    sources_ref,
    diag_ref,
    inverse_ref,
    load_ref,
    stage,
    c_high,
    c_low,
    t_high,
    t_low,
    rhs,
    turned,
    loads_ref,
    x_ref,
    image,
    residual,
    direction,
    interior,
    diag_full,
    w_send,
    w_recv,
    c_send,
    c_full,
    half_send,
    half_recv,
    far_send,
    far_recv,
    own_part,
    near_send,
    near_recv,
    merged,
    piece_sums,
    tr_ref,
    td_ref,
    rr_ref,
    q_send,
    q_recv,
    g_send,
    g_recv,
    load_sem,
    stage_sem,
    w_ssem,
    w_rsem,
    c_ssem,
    c_rsem,
    h_ssem,
    h_rsem,
    f_ssem,
    f_rsem,
    n_ssem,
    n_rsem,
    m_ssem,
    m_rsem,
    p_ssem,
    p_rsem,
    q_ssem,
    q_rsem,
    g_ssem,
    g_rsem,
):
    nz, ny, nx = grid
    fronts, leaves = nz * ny, nx * CORES
    rows, cols = loads_ref.shape
    depth = stage.shape[1]
    rank = inverse_ref.shape[1]
    piece = rows // 2 // nx
    tile, lanes = 128, cols // 2
    half_rank, half_piece = rank // 2, piece // 2
    streams = range(STREAMS)
    front = lax.axis_index("front")
    leaf = lax.axis_index("leaf")
    z, y = front // ny, front % ny
    x, core = leaf // CORES, leaf % CORES
    partner, other = x * CORES + (1 - core), 1 - core

    z_steps, y_steps = far_first(nz), far_first(ny)
    far = nx // 2
    near = [d for d in range(1, nx) if d != far]
    peers = [(dz, dy) for dz in z_steps for dy in y_steps if dz or dy]

    def front_at(dz, dy):
        return ((z + dz) % nz) * ny + (y + dy) % ny

    def leaf_at(dx, at_core):
        return ((x + dx) % nx) * CORES + at_core

    def piece_at(dx, at_core):
        return at_core * nx + (x + dx) % nx

    def remote(source, target, sems, at, **place):
        return pltpu.make_async_remote_copy(
            src_ref=source,
            dst_ref=target,
            send_sem=sems[0].at[at],
            recv_sem=sems[1].at[at],
            device_id=place,
        )

    def send(*args, **place):
        copy = remote(*args, **place)
        copy.start()
        return copy

    def swap(value):
        return pltpu.roll(value, lanes, 1)

    def select(a, b):
        return jnp.where(lax.broadcasted_iota(jnp.int32, a.shape, 1) < lanes, a, b)

    def packed(value, s):
        top, bottom = jnp.split(value, 2)
        return select(top, swap(bottom)) if s == 0 else select(swap(top), bottom)

    def full(a, b):
        return jnp.concatenate([select(a, swap(b)), select(swap(a), b)])

    def fold(products):
        top, bottom = jnp.split(products + swap(products), 2)
        return select(top, bottom)

    def operand(value):
        high = value.astype(BF16).astype(F32)
        low = value - high
        return jnp.concatenate([select(high, swap(low)), select(swap(high), low)]).astype(BF16)

    def both_sides(row):
        return row + swap(row)

    loads = [
        pltpu.make_async_copy(source, here, load_sem.at[i])
        for i, (source, here) in enumerate(
            (
                (order_hbm, order_ref),
                (sources_hbm, sources_ref),
                (diag_hbm, diag_ref),
                (inverse_hbm, inverse_ref),
                (load_hbm, load_ref),
            )
        )
    ]
    for copy in loads[:2]:
        copy.start()
    stages = []
    step_rows = rows // stage_sem.shape[0]
    for i in range(stage_sem.shape[0]):
        part = pl.ds(i * step_rows, step_rows)
        stages.append(
            pltpu.make_async_copy(coupling_hbm.at[part], stage.at[part], stage_sem.at[i])
        )
        stages[-1].start()
    for copy in loads[2:]:
        copy.start()

    barrier = pltpu.get_barrier_semaphore()
    for dz, dy in peers:
        pl.semaphore_signal(barrier, inc=1, device_id={"front": front_at(dz, dy)})
    for d in range(1, leaves):
        pl.semaphore_signal(barrier, inc=1, device_id={"leaf": (leaf + d) % leaves})

    def products(s, n, im, others):
        for i, field in enumerate(others):
            piece_sums[s, n, i] = (field * im).reshape(-1, 8, cols).sum(axis=0)

    for copy in loads[:2]:
        copy.wait()

    def take(i, _):
        for j in range(16):
            at = i * 16 + j
            loads_ref[pl.ds(at, 1), :] = sources_ref[pl.ds(order_ref[at] & (rows - 1), 1), :]
        return 0

    lax.fori_loop(0, rows // 16, take, 0)
    for i in range(0, rows, tile):
        high, low = split(loads_ref[i : i + tile, :].T)
        turned[0:cols, i : i + tile] = high
        turned[cols:, i : i + tile] = low

    def start_fields(n, _):
        block = loads_ref[pl.ds(pl.multiple_of(n * piece, piece), piece), :]
        at = pl.ds(pl.multiple_of(n * half_piece, half_piece), half_piece)
        for s in streams:
            value = packed(block, s)
            image[s, at, :] = value
            residual[s, at, :] = value
            direction[s, at, :] = value
            x_ref[s, at, :] = jnp.zeros_like(value)
            products(s, n, value, (value,) * SUMS)
        return 0

    lax.fori_loop(0, rows // piece, start_fields, 0)

    for i, copy in enumerate(stages):
        copy.wait()

        def divide(j, _, i=i):
            at = pl.ds(pl.multiple_of(i * step_rows + j * 16, 16), 16)
            high, low = split(stage[at, :])
            c_high[at, :] = high
            c_low[at, :] = low
            return 0

        lax.fori_loop(0, step_rows // 16, divide, 0)

    def turn(start, stop):
        def columns(j, _):
            for r in range(start, stop, tile):
                at = pl.ds(pl.multiple_of(j * tile, tile), tile)
                high, low = split(stage[r : r + tile, at].T)
                t_high[at, r : r + tile] = high
                t_low[at, r : r + tile] = low
            return 0

        lax.fori_loop(0, depth // tile, columns, 0)

    def spread_diagonal():
        for n in range(rows // piece):
            first = n * piece
            row = diag_ref[first // tile : first // tile + 1, first % tile : first % tile + piece]
            column = jnp.broadcast_to(row, (tile, piece)).T
            at = slice(n * half_piece, (n + 1) * half_piece)
            diag_full[at, :] = select(column[:half_piece], column[half_piece:])

    def start_interior():
        for n in range(fronts):
            value = jnp.dot(
                inverse_ref[n], load_ref[n], precision=HIGHEST, preferred_element_type=F32
            )
            for s in streams:
                interior[s, n * half_rank : (n + 1) * half_rank, :] = packed(value, s)

    pl.semaphore_wait(barrier, len(peers) + leaves - 1)

    def times(high_ref, low_ref, s, starts, size):
        unit = size // 2
        units = [pl.ds(pl.multiple_of(at + i, unit), unit) for at in starts for i in (0, unit)]
        both = []
        for part in (units[: len(starts)], units[len(starts) :]):
            high = jnp.concatenate([high_ref[at, :] for at in part])
            low = jnp.concatenate([low_ref[at, :] for at in part])
            out = jnp.dot(high, rhs[s], preferred_element_type=F32)
            both.append(out + jnp.dot(low, rhs[s], preferred_element_type=F32))
        return jnp.concatenate(both)

    def times_turned():
        n = depth // 2
        both = []
        for i in (0, n):
            at = slice(i, i + n)
            out = jnp.dot(turned[...], c_high[:, at], preferred_element_type=F32)
            both.append(out + jnp.dot(turned[...], c_low[:, at], preferred_element_type=F32))
        both = [out[:cols] + out[cols:] for out in both]
        return jnp.concatenate([out[:, i : i + tile].T for out in both for i in range(0, n, tile)])

    def arrived(s, n):
        at = pl.ds(pl.multiple_of(n * half_piece, half_piece), half_piece)
        along = direction[s, at, :]
        new = diag_full[at, :] * along + merged[s, n]
        image[s, at, :] = new
        rhs[s, pl.ds(pl.multiple_of(n * piece, piece), piece), :] = operand(new)
        products(s, n, new, (along, residual[s, at, :], new))

    size = half_rank + SUMS

    def projection(s, dz, dy):
        to = front_at(dz, dy)
        return remote(
            w_send.at[s, to, 0:size],
            w_recv.at[s, front, 0:size],
            (w_ssem, w_rsem),
            (s, dz * ny + dy),
            front=to,
        )

    def sums_of(s):
        sums = [piece_sums[s, 0, n] for n in range(SUMS)]
        for i in range(1, rows // piece):
            sums = [total + piece_sums[s, i, n] for n, total in enumerate(sums)]
        sums = [both_sides(total.sum(axis=0, keepdims=True)) for total in sums]
        return jnp.concatenate(sums + [jnp.zeros((EXTRA - SUMS, cols), F32)])

    def project_first():
        out = times_turned()
        for s in streams:
            dots = sums_of(s)
            for j in range(fronts):
                w_send[s, j, 0:half_rank, :] = packed(out[j * rank : (j + 1) * rank], s)
                w_send[s, j, half_rank:, :] = dots
            for dz, dy in peers:
                projection(s, dz, dy).start()

    def project(s):
        dots = sums_of(s)
        span = ny * rank
        for i in range(0, nz, 2):
            steps = z_steps[i : i + 2]
            places = [(z + dz) % nz for dz in steps]
            out = times(t_high, t_low, s, [p * span for p in places], span)
            for n, place in enumerate(places):
                for j in range(ny):
                    at = n * span + j * rank
                    w_send[s, place * ny + j, 0:half_rank, :] = fold(out[at : at + rank])
                    w_send[s, place * ny + j, half_rank:, :] = dots
            for dz in steps:
                for dy in y_steps:
                    if dz or dy:
                        projection(s, dz, dy).start()

    def condense(s, k, is_first):
        w_recv[s, front, 0:size, :] = w_send[s, front, 0:size, :]
        if is_first and s == 0:
            turn(0, rows // 2)
            loads[3].wait()
        for dz, dy in peers:
            projection(s, dz, dy).wait_recv()
        total = w_recv[s, 0]
        for n in range(1, fronts):
            total = total + w_recv[s, n]
        w = total[0:half_rank]
        curvature, cross, square = (total[half_rank + n : half_rank + n + 1] for n in range(SUMS))
        if is_first:
            alpha = beta = None
            rr_ref[s] = square
            tr = td = w
        else:
            rr = rr_ref[s]
            alpha = rr / curvature
            rr_next = rr - 2.0 * alpha * cross + alpha * alpha * square
            beta = rr_next / rr
            rr_ref[s] = rr_next
            tr = tr_ref[s] - alpha * w
            td = tr + beta * td_ref[s]
        tr_ref[s] = tr
        td_ref[s] = td
        coeff = jnp.dot(
            inverse_ref[front],
            jnp.concatenate([td, swap(td)]),
            precision=HIGHEST,
            preferred_element_type=F32,
        )
        coeff = packed(coeff, 0)
        here = pl.ds(pl.multiple_of(front * half_rank, half_rank), half_rank)
        c_send[s] = coeff
        c_full[k, s, here, :] = coeff
        spread = [
            send(
                c_send.at[s],
                c_full.at[k, s, here],
                (c_ssem, c_rsem),
                (s, dz * ny + dy),
                front=front_at(dz, dy),
            )
            for dz, dy in peers
        ]
        return alpha, beta, (td * coeff).reshape(-1, 8, cols).sum(axis=0), spread

    def advance(s, alpha, beta):
        for i in range(0, rows // 2, tile):
            at = slice(i, i + tile)
            x_ref[s, at, :] += alpha * direction[s, at, :]
            res = residual[s, at, :] - alpha * image[s, at, :]
            residual[s, at, :] = res
            direction[s, at, :] = res + beta * direction[s, at, :]

    def subtract(s, k, step):
        for i in range(0, depth // 2, tile):
            at = slice(i, i + tile)
            interior[s, at, :] = interior[s, at, :] - step * c_full[k, s, at, :]

    def finish(s, k, alpha, beta, is_first):
        if not is_first:
            advance(s, alpha, beta)
            subtract(s, k - 1, alpha)
        elif s == 0:
            for copy in (loads[2], loads[4]):
                copy.wait()
            turn(rows // 2, rows)
        else:
            spread_diagonal()
            start_interior()
        for dz, dy in peers:
            projection(s, dz, dy).wait_send()

    def merge(s, k, spread):
        for copy in spread:
            copy.wait_recv()
        for n in range(fronts):
            rhs[s, n * rank : (n + 1) * rank, :] = operand(
                c_full[k, s, n * half_rank : (n + 1) * half_rank, :]
            )

        def field(pieces):
            out = times(c_high, c_low, s, [n * piece for n in pieces], piece)
            return [fold(out[i * piece : (i + 1) * piece]) for i in range(len(pieces))]

        sent = []
        ends = (other, core)
        for at_core, value in zip(ends, field([piece_at(far, n) for n in ends])):
            far_send[s, at_core] = value
        for n, at_core in enumerate(ends):
            sent.append(
                send(
                    far_send.at[s, at_core],
                    far_recv.at[s, core],
                    (f_ssem, f_rsem),
                    (s, 1 - n),
                    leaf=leaf_at(far, at_core),
                )
            )
        steps = near + [0]
        for d, value in zip(steps, field([piece_at(d, other) for d in steps])):
            half_send[s, d] = value
        swapped = [
            send(half_send.at[s, d], half_recv.at[s, d], (h_ssem, h_rsem), (s, d), leaf=partner)
            for d in steps
        ]
        for d, value in zip(steps, field([piece_at(d, core) for d in steps])):
            own_part[s, d] = value
        for copy in spread:
            copy.wait_send()
        for d, copy in zip(steps, swapped):
            copy.wait_recv()
            if d:
                near_send[s, d] = own_part[s, d] + half_recv[s, d]
                sent.append(
                    send(
                        near_send.at[s, d],
                        near_recv.at[s, d],
                        (n_ssem, n_rsem),
                        (s, d),
                        leaf=leaf_at(d, core),
                    )
                )
        return sent, swapped

    def gather(s, sent, swapped):
        total = own_part[s, 0] + half_recv[s, 0]
        for copy in sent:
            copy.wait_recv()
        for d in near:
            total = total + near_recv[s, d]
        for n in range(CORES):
            total = total + far_recv[s, n]
        mine = piece_at(0, core)
        merged[s, mine] = total
        here = merged.at[s, mine]
        gathered = {
            d: send(here, here, (m_ssem, m_rsem), (s, d), leaf=leaf_at(d, core))
            for d in [far] + near
        }
        passed = {0: send(here, here, (p_ssem, p_rsem), (s, 0), leaf=partner)}
        arrived(s, mine)
        for copy in sent + swapped:
            copy.wait_send()
        return gathered, passed

    def collect(s, gathered, passed):
        passed[0].wait_recv()
        arrived(s, piece_at(0, other))
        for d in near + [far]:
            gathered[d].wait_recv()
            at = merged.at[s, piece_at(nx - d, core)]
            passed[d] = send(at, at, (p_ssem, p_rsem), (s, d), leaf=partner)
            arrived(s, piece_at(nx - d, core))
        for d in near + [far]:
            passed[d].wait_recv()
            arrived(s, piece_at(nx - d, other))
        for copy in list(gathered.values()) + list(passed.values()):
            copy.wait_send()

    def iterate(k, is_first):
        spreads = []
        for s in streams:
            alpha, beta, _, spread = condense(s, k, is_first)
            spreads.append(spread)
            finish(s, k, alpha, beta, is_first)
        moves = [merge(s, k, spreads[s]) for s in streams]
        moves = [gather(s, *moves[s]) for s in streams]
        for s in streams:
            collect(s, *moves[s])
            project(s)
        return 0

    project_first()
    iterate(0, True)
    lax.fori_loop(1, ITERS - 1, lambda k, _: iterate(k, False), 0)

    end = ITERS - 1
    ends = [condense(s, end, False) for s in streams]

    def both_streams(values):
        return select(*(both_sides(value) for value in values))

    own = both_streams([own for _, _, own, _ in ends])
    q_send[...] = own
    q_recv[leaf] = own
    over_leaf = [
        send(
            q_send, q_recv.at[leaf], (q_ssem, q_rsem), d, leaf=(leaf + d) % leaves
        )
        for d in range(1, leaves)
    ]
    totals = []
    for s, (alpha, beta, _, _) in enumerate(ends):
        advance(s, alpha, beta)
        q = jnp.zeros((8, cols), F32)
        for i in range(0, rows // 2, tile):
            new = direction[s, i : i + tile, :]
            q = q + (diag_full[i : i + tile, :] * new * new).reshape(-1, 8, cols).sum(axis=0)
        totals.append(q)
    q = both_streams(totals)
    for copy in over_leaf:
        copy.wait_recv()
    for n in range(leaves):
        q = q + q_recv[n]
    g_send[...] = q
    g_recv[front] = q
    over_front = [
        send(
            g_send,
            g_recv.at[front],
            (g_ssem, g_rsem),
            dz * ny + dy,
            front=front_at(dz, dy),
        )
        for dz, dy in peers
    ]
    for s, (alpha, _, _, _) in enumerate(ends):
        subtract(s, end - 1, alpha)

    def widen(n, _):
        at = pl.ds(pl.multiple_of(n * half_piece, half_piece), half_piece)
        to = pl.ds(pl.multiple_of(n * piece, piece), piece)
        x_out[to, :] = full(x_ref[0, at, :], x_ref[1, at, :])
        direction_out[to, :] = full(direction[0, at, :], direction[1, at, :])
        return 0

    lax.fori_loop(0, rows // piece, widen, 0)

    def widen_interior(n, _):
        at = pl.ds(pl.multiple_of(n * half_rank, half_rank), half_rank)
        to = pl.ds(pl.multiple_of(n * rank, rank), rank)
        interior_out[to, :] = full(interior[0, at, :], interior[1, at, :])
        return 0

    lax.fori_loop(0, fronts, widen_interior, 0)
    for s, (_, _, _, spread) in enumerate(ends):
        for dz, dy in peers:
            projection(s, dz, dy).wait_send()
        for copy in spread:
            copy.wait_recv()
    for n in range(fronts):
        at = slice(n * half_rank, (n + 1) * half_rank)
        last_out[n * rank : (n + 1) * rank, :] = full(c_full[end, 0, at, :], c_full[end, 1, at, :])
    for copy in over_front:
        copy.wait_recv()
    q = g_recv[0]
    for n in range(1, fronts):
        q = q + g_recv[n]
    step_ref[...] = select(rr_ref[0], rr_ref[1]) / q.sum(axis=0, keepdims=True)
    for _, _, _, spread in ends:
        for copy in spread:
            copy.wait_send()
    for copy in over_leaf + over_front:
        copy.wait_send()


def per_device(sources, order, diagonal, coupling, interior_inverse, interior_load, grid=(NZ, NY, NX)):
    nz, ny, nx = grid
    fronts, leaves = nz * ny, nx * CORES
    rows, cols = sources.shape
    depth = coupling.shape[1]
    blocks, rank = interior_inverse.shape[:2]
    assert blocks == fronts and depth == blocks * rank
    piece = rows // 2 // nx
    vmem = pl.BlockSpec(memory_space=pltpu.VMEM)
    dma = pltpu.SemaphoreType.DMA
    field = pltpu.VMEM((rows, cols), F32)
    halves = pltpu.VMEM((STREAMS, rows // 2, cols), F32)
    hbm = pl.BlockSpec(memory_space=pltpu.HBM)
    whole = jax.ShapeDtypeStruct((rows, cols), F32)
    inner = jax.ShapeDtypeStruct((depth, cols), F32)
    x, direction, interior, coeff, step = pl.pallas_call(
        functools.partial(front_solve, grid),
        out_shape=(whole, whole, inner, inner, jax.ShapeDtypeStruct((1, cols), F32)),
        in_specs=[hbm] * 6,
        out_specs=(vmem,) * 5,
        scratch_shapes=[
            pltpu.SMEM((rows,), jnp.int32),
            field,
            pltpu.VMEM((rows // 128, 128), F32),
            pltpu.VMEM(interior_inverse.shape, F32),
            pltpu.VMEM(interior_load.shape, F32),
            pltpu.VMEM((rows, depth), F32),
            pltpu.VMEM((rows, depth), BF16),
            pltpu.VMEM((rows, depth), BF16),
            pltpu.VMEM((depth, rows), BF16),
            pltpu.VMEM((depth, rows), BF16),
            pltpu.VMEM((STREAMS, max(rows, depth), cols), BF16),
            pltpu.VMEM((2 * cols, rows), BF16),
            field,
            halves,
            halves,
            halves,
            halves,
            pltpu.VMEM((STREAMS, depth // 2, cols), F32),
            pltpu.VMEM((rows // 2, cols), F32),
            pltpu.VMEM((STREAMS, fronts, rank // 2 + EXTRA, cols), F32),
            pltpu.VMEM((STREAMS, fronts, rank // 2 + EXTRA, cols), F32),
            pltpu.VMEM((STREAMS, rank // 2, cols), F32),
            pltpu.VMEM((ITERS, STREAMS, depth // 2, cols), F32),
            pltpu.VMEM((STREAMS, nx, piece // 2, cols), F32),
            pltpu.VMEM((STREAMS, nx, piece // 2, cols), F32),
            pltpu.VMEM((STREAMS, CORES, piece // 2, cols), F32),
            pltpu.VMEM((STREAMS, CORES, piece // 2, cols), F32),
            pltpu.VMEM((STREAMS, nx, piece // 2, cols), F32),
            pltpu.VMEM((STREAMS, nx, piece // 2, cols), F32),
            pltpu.VMEM((STREAMS, nx, piece // 2, cols), F32),
            pltpu.VMEM((STREAMS, CORES * nx, piece // 2, cols), F32),
            pltpu.VMEM((STREAMS, CORES * nx, SUMS, 8, cols), F32),
            pltpu.VMEM((STREAMS, rank // 2, cols), F32),
            pltpu.VMEM((STREAMS, rank // 2, cols), F32),
            pltpu.VMEM((STREAMS, 1, cols), F32),
            pltpu.VMEM((8, cols), F32),
            pltpu.VMEM((leaves, 8, cols), F32),
            pltpu.VMEM((8, cols), F32),
            pltpu.VMEM((fronts, 8, cols), F32),
            dma((5,)),
            dma((min(8, rows // 128),)),
            dma((STREAMS, fronts)),
            dma((STREAMS, fronts)),
            dma((STREAMS, fronts)),
            dma((STREAMS, fronts)),
            dma((STREAMS, nx)),
            dma((STREAMS, nx)),
            dma((STREAMS, CORES)),
            dma((STREAMS, CORES)),
            dma((STREAMS, nx)),
            dma((STREAMS, nx)),
            dma((STREAMS, nx)),
            dma((STREAMS, nx)),
            dma((STREAMS, nx)),
            dma((STREAMS, nx)),
            dma((leaves,)),
            dma((leaves,)),
            dma((fronts,)),
            dma((fronts,)),
        ],
        compiler_params=pltpu.CompilerParams(
            collective_id=0, has_side_effects=True, vmem_limit_bytes=48 << 20
        ),
        name="front_solve",
    )(
        *(
            pltpu.with_memory_space_constraint(value, pltpu.HBM)
            for value in (
                order,
                sources,
                diagonal.reshape(rows // 128, 128),
                coupling,
                interior_inverse,
                interior_load,
            )
        )
    )
    interior = interior - step * coeff
    return x + step * direction, interior.reshape(interior_load.shape)


def solution(mesh):
    in_specs = (
        P(("wave", "front"), None),
        P("front"),
        P(("wave", "front")),
        P(("wave", "front"), "leaf"),
        P(("wave", "leaf"), None, None),
        P(("wave", "leaf"), None, None),
    )
    out_specs = (P(("wave", "front"), None), P(("wave", "leaf"), None, None))
    return jax.shard_map(
        per_device, mesh=mesh, in_specs=in_specs, out_specs=out_specs, check_vma=False
    )
```

```python
import functools

import jax
import jax.numpy as jnp
from jax import lax
from jax.experimental import pallas as pl
from jax.experimental.pallas import tpu as pltpu
from jax.sharding import PartitionSpec as P

ITERS = 4
NZ, NY, NX, CORES = 4, 4, 4, 2
EXTRA = 8
SUMS = 3
STREAMS = 2
HIGHEST = lax.Precision.HIGHEST
F32 = jnp.float32
BF16 = jnp.bfloat16


def far_first(n):
    return sorted(range(n), key=lambda d: -min(d, n - d))


def split(value):
    high = value.astype(BF16)
    return high, (value - high.astype(F32)).astype(BF16)


def front_solve(
    grid,
    order_hbm,
    sources_hbm,
    diag_hbm,
    coupling_hbm,
    inverse_hbm,
    load_hbm,
    x_out,
    direction_out,
    interior_out,
    last_out,
    step_ref,
    order_ref,
    sources_ref,
    diag_ref,
    inverse_ref,
    load_ref,
    stage,
    c_high,
    c_low,
    t_high,
    t_low,
    rhs,
    turned,
    loads_ref,
    x_ref,
    image,
    residual,
    direction,
    interior,
    diag_full,
    w_send,
    w_recv,
    c_send,
    c_full,
    half_send,
    half_recv,
    far_send,
    far_recv,
    own_part,
    near_send,
    near_recv,
    merged,
    piece_sums,
    tr_ref,
    td_ref,
    rr_ref,
    q_send,
    q_recv,
    g_send,
    g_recv,
    load_sem,
    stage_sem,
    w_ssem,
    w_rsem,
    c_ssem,
    c_rsem,
    h_ssem,
    h_rsem,
    f_ssem,
    f_rsem,
    n_ssem,
    n_rsem,
    m_ssem,
    m_rsem,
    o_ssem,
    o_rsem,
    p_ssem,
    p_rsem,
    q_ssem,
    q_rsem,
    g_ssem,
    g_rsem,
):
    nz, ny, nx = grid
    fronts, leaves = nz * ny, nx * CORES
    rows, cols = loads_ref.shape
    depth = stage.shape[1]
    rank = inverse_ref.shape[1]
    piece = rows // 2 // nx
    tile, lanes = 128, cols // 2
    half_rank, half_piece = rank // 2, piece // 2
    streams = range(STREAMS)
    front = lax.axis_index("front")
    leaf = lax.axis_index("leaf")
    z, y = front // ny, front % ny
    x, core = leaf // CORES, leaf % CORES
    partner, other = x * CORES + (1 - core), 1 - core

    z_steps, y_steps = far_first(nz), far_first(ny)
    far = nx // 2
    near = [d for d in range(1, nx) if d != far]
    peers = [(dz, dy) for dz in z_steps for dy in y_steps if dz or dy]

    def front_at(dz, dy):
        return ((z + dz) % nz) * ny + (y + dy) % ny

    def leaf_at(dx, at_core):
        return ((x + dx) % nx) * CORES + at_core

    def piece_at(dx, at_core):
        return at_core * nx + (x + dx) % nx

    def remote(source, target, sems, at, **place):
        return pltpu.make_async_remote_copy(
            src_ref=source,
            dst_ref=target,
            send_sem=sems[0].at[at],
            recv_sem=sems[1].at[at],
            device_id=place,
        )

    def send(*args, **place):
        copy = remote(*args, **place)
        copy.start()
        return copy

    def swap(value):
        return pltpu.roll(value, lanes, 1)

    def select(a, b):
        return jnp.where(lax.broadcasted_iota(jnp.int32, a.shape, 1) < lanes, a, b)

    def packed(value, s):
        top, bottom = jnp.split(value, 2)
        return select(top, swap(bottom)) if s == 0 else select(swap(top), bottom)

    def full(a, b):
        return jnp.concatenate([select(a, swap(b)), select(swap(a), b)])

    def fold(products):
        top, bottom = jnp.split(products + swap(products), 2)
        return select(top, bottom)

    def operand(value):
        high = value.astype(BF16).astype(F32)
        low = value - high
        return jnp.concatenate([select(high, swap(low)), select(swap(high), low)]).astype(BF16)

    def both_sides(row):
        return row + swap(row)

    loads = [
        pltpu.make_async_copy(source, here, load_sem.at[i])
        for i, (source, here) in enumerate(
            (
                (order_hbm, order_ref),
                (sources_hbm, sources_ref),
                (diag_hbm, diag_ref),
                (inverse_hbm, inverse_ref),
                (load_hbm, load_ref),
            )
        )
    ]
    for copy in loads[:2]:
        copy.start()
    stages = []
    step_rows = rows // stage_sem.shape[0]
    for i in range(stage_sem.shape[0]):
        part = pl.ds(i * step_rows, step_rows)
        stages.append(
            pltpu.make_async_copy(coupling_hbm.at[part], stage.at[part], stage_sem.at[i])
        )
        stages[-1].start()
    for copy in loads[2:]:
        copy.start()

    barrier = pltpu.get_barrier_semaphore()
    for dz, dy in peers:
        pl.semaphore_signal(barrier, inc=1, device_id={"front": front_at(dz, dy)})
    for d in range(1, leaves):
        pl.semaphore_signal(barrier, inc=1, device_id={"leaf": (leaf + d) % leaves})

    def products(s, n, im, others):
        for i, field in enumerate(others):
            piece_sums[s, n, i] = (field * im).reshape(-1, 8, cols).sum(axis=0)

    for copy in loads[:2]:
        copy.wait()

    for i, copy in enumerate(stages):
        copy.wait()

        def prepare(j, _, i=i):
            first = i * step_rows + j * 16
            at = pl.ds(pl.multiple_of(first, 16), 16)
            high, low = split(stage[at, :])
            c_high[at, :] = high
            c_low[at, :] = low
            for n in range(16):
                row = pl.ds(order_ref[first + n] & (rows - 1), 1)
                loads_ref[pl.ds(first + n, 1), :] = sources_ref[row, :]
            return 0

        lax.fori_loop(0, step_rows // 16, prepare, 0)
    square = jnp.zeros((8, cols), F32)
    for i in range(0, rows, tile):
        high, low = split(loads_ref[i : i + tile, :].T)
        turned[0:cols, i : i + tile] = high
        turned[cols:, i : i + tile] = low
        block = loads_ref[i : i + tile, :]
        square = square + (block * block).reshape(-1, 8, cols).sum(axis=0)
    square = square.sum(axis=0, keepdims=True)

    def start_fields(n, _):
        block = loads_ref[pl.ds(pl.multiple_of(n * piece, piece), piece), :]
        at = pl.ds(pl.multiple_of(n * half_piece, half_piece), half_piece)
        for s in streams:
            value = packed(block, s)
            image[s, at, :] = value
            residual[s, at, :] = value
            direction[s, at, :] = value
            x_ref[s, at, :] = jnp.zeros_like(value)
        return 0

    def turn(start, stop):
        def columns(j, _):
            for r in range(start, stop, tile):
                at = pl.ds(pl.multiple_of(j * tile, tile), tile)
                high, low = split(stage[r : r + tile, at].T)
                t_high[at, r : r + tile] = high
                t_low[at, r : r + tile] = low
            return 0

        lax.fori_loop(0, depth // tile, columns, 0)

    def spread_diagonal():
        for n in range(rows // piece):
            first = n * piece
            row = diag_ref[first // tile : first // tile + 1, first % tile : first % tile + piece]
            column = jnp.broadcast_to(row, (tile, piece)).T
            at = slice(n * half_piece, (n + 1) * half_piece)
            diag_full[at, :] = select(column[:half_piece], column[half_piece:])

    def start_interior():
        for n in range(fronts):
            value = jnp.dot(
                inverse_ref[n], load_ref[n], precision=HIGHEST, preferred_element_type=F32
            )
            for s in streams:
                interior[s, n * half_rank : (n + 1) * half_rank, :] = packed(value, s)

    pl.semaphore_wait(barrier, len(peers) + leaves - 1)

    def times(high_ref, low_ref, s, starts, size):
        unit = size // 2
        units = [pl.ds(pl.multiple_of(at + i, unit), unit) for at in starts for i in (0, unit)]
        both = []
        for part in (units[: len(starts)], units[len(starts) :]):
            high = jnp.concatenate([high_ref[at, :] for at in part])
            low = jnp.concatenate([low_ref[at, :] for at in part])
            out = jnp.dot(high, rhs[s], preferred_element_type=F32)
            both.append(out + jnp.dot(low, rhs[s], preferred_element_type=F32))
        return jnp.concatenate(both)

    def times_turned():
        n = depth // 2
        both = []
        for i in (0, n):
            at = slice(i, i + n)
            out = jnp.dot(turned[...], c_high[:, at], preferred_element_type=F32)
            both.append(out + jnp.dot(turned[...], c_low[:, at], preferred_element_type=F32))
        both = [out[:cols] + out[cols:] for out in both]
        return jnp.concatenate([out[:, i : i + tile].T for out in both for i in range(0, n, tile)])

    def arrived(s, n):
        at = pl.ds(pl.multiple_of(n * half_piece, half_piece), half_piece)
        along = direction[s, at, :]
        new = diag_full[at, :] * along + merged[s, n]
        image[s, at, :] = new
        rhs[s, pl.ds(pl.multiple_of(n * piece, piece), piece), :] = operand(new)
        products(s, n, new, (along, residual[s, at, :], new))

    size = half_rank + SUMS

    def projection(s, dz, dy):
        to = front_at(dz, dy)
        return remote(
            w_send.at[s, to, 0:size],
            w_recv.at[s, front, 0:size],
            (w_ssem, w_rsem),
            (s, dz * ny + dy),
            front=to,
        )

    def sums_of(s):
        sums = [piece_sums[s, 0, n] for n in range(SUMS)]
        for i in range(1, rows // piece):
            sums = [total + piece_sums[s, i, n] for n, total in enumerate(sums)]
        sums = [both_sides(total.sum(axis=0, keepdims=True)) for total in sums]
        return jnp.concatenate(sums + [jnp.zeros((EXTRA - SUMS, cols), F32)])

    def project_first():
        out = times_turned()
        for s in streams:
            norm = select(square, swap(square)) if s == 0 else select(swap(square), square)
            dots = jnp.concatenate([norm] * SUMS + [jnp.zeros((EXTRA - SUMS, cols), F32)])
            for j in range(fronts):
                w_send[s, j, 0:half_rank, :] = packed(out[j * rank : (j + 1) * rank], s)
                w_send[s, j, half_rank:, :] = dots
            for dz, dy in peers:
                projection(s, dz, dy).start()
        lax.fori_loop(0, rows // piece, start_fields, 0)

    def project(s, between=None):
        dots = sums_of(s)
        span = ny * rank
        for i in range(0, nz, 2):
            steps = z_steps[i : i + 2]
            places = [(z + dz) % nz for dz in steps]
            out = times(t_high, t_low, s, [p * span for p in places], span)
            for n, place in enumerate(places):
                for j in range(ny):
                    at = n * span + j * rank
                    w_send[s, place * ny + j, 0:half_rank, :] = fold(out[at : at + rank])
                    w_send[s, place * ny + j, half_rank:, :] = dots
            for dz in steps:
                for dy in y_steps:
                    if dz or dy:
                        projection(s, dz, dy).start()
            if between and i:
                between()

    def condense(s, k, is_first):
        w_recv[s, front, 0:size, :] = w_send[s, front, 0:size, :]
        if is_first and s == 0:
            turn(0, rows // 2)
            loads[3].wait()
        for dz, dy in peers:
            projection(s, dz, dy).wait_recv()
        total = w_recv[s, 0]
        for n in range(1, fronts):
            total = total + w_recv[s, n]
        w = total[0:half_rank]
        curvature, cross, square = (total[half_rank + n : half_rank + n + 1] for n in range(SUMS))
        if is_first:
            alpha = beta = None
            rr_ref[s] = square
            tr = td = w
        else:
            rr = rr_ref[s]
            alpha = rr / curvature
            rr_next = rr - 2.0 * alpha * cross + alpha * alpha * square
            beta = rr_next / rr
            rr_ref[s] = rr_next
            tr = tr_ref[s] - alpha * w
            td = tr + beta * td_ref[s]
        tr_ref[s] = tr
        td_ref[s] = td
        coeff = jnp.dot(
            inverse_ref[front],
            jnp.concatenate([td, swap(td)]),
            precision=HIGHEST,
            preferred_element_type=F32,
        )
        coeff = packed(coeff, 0)
        here = pl.ds(pl.multiple_of(front * half_rank, half_rank), half_rank)
        c_send[s] = coeff
        c_full[k, s, here, :] = coeff
        spread = [
            send(
                c_send.at[s],
                c_full.at[k, s, here],
                (c_ssem, c_rsem),
                (s, dz * ny + dy),
                front=front_at(dz, dy),
            )
            for dz, dy in peers
        ]
        return alpha, beta, (td * coeff).reshape(-1, 8, cols).sum(axis=0), spread

    def advance(s, alpha, beta):
        for i in range(0, rows // 2, tile):
            at = slice(i, i + tile)
            x_ref[s, at, :] += alpha * direction[s, at, :]
            res = residual[s, at, :] - alpha * image[s, at, :]
            residual[s, at, :] = res
            direction[s, at, :] = res + beta * direction[s, at, :]

    def subtract(s, k, step):
        for i in range(0, depth // 2, tile):
            at = slice(i, i + tile)
            interior[s, at, :] = interior[s, at, :] - step * c_full[k, s, at, :]

    def finish(s, k, alpha, beta, is_first):
        if not is_first:
            advance(s, alpha, beta)
            subtract(s, k - 1, alpha)
        elif s == 0:
            for copy in (loads[2], loads[4]):
                copy.wait()
            turn(rows // 2, rows)
        else:
            spread_diagonal()
            start_interior()
        for dz, dy in peers:
            projection(s, dz, dy).wait_send()

    def merge(s, k, spread):
        for copy in spread:
            copy.wait_recv()
        for n in range(fronts):
            rhs[s, n * rank : (n + 1) * rank, :] = operand(
                c_full[k, s, n * half_rank : (n + 1) * half_rank, :]
            )

        def field(pieces):
            out = times(c_high, c_low, s, [n * piece for n in pieces], piece)
            return [fold(out[i * piece : (i + 1) * piece]) for i in range(len(pieces))]

        def swap_over(d):
            return send(
                half_send.at[s, d], half_recv.at[s, d], (h_ssem, h_rsem), (s, d), leaf=partner
            )

        swapped = {}
        if near:
            for d, value in zip(near, field([piece_at(d, other) for d in near])):
                half_send[s, d] = value
            for d in near:
                swapped[d] = swap_over(d)
        sent = []
        ends = (other, core)
        for at_core, value in zip(ends, field([piece_at(far, n) for n in ends])):
            far_send[s, at_core] = value
        for n, at_core in enumerate(ends):
            sent.append(
                send(
                    far_send.at[s, at_core],
                    far_recv.at[s, core],
                    (f_ssem, f_rsem),
                    (s, 1 - n),
                    leaf=leaf_at(far, at_core),
                )
            )
        steps = near + [0]
        values = field([piece_at(0, other)] + [piece_at(d, core) for d in steps])
        half_send[s, 0] = values[0]
        swapped[0] = swap_over(0)
        for d, value in zip(steps, values[1:]):
            own_part[s, d] = value
        for d in near:
            swapped[d].wait_recv()
            near_send[s, d] = own_part[s, d] + half_recv[s, d]
            sent.append(
                send(
                    near_send.at[s, d],
                    near_recv.at[s, d],
                    (n_ssem, n_rsem),
                    (s, d),
                    leaf=leaf_at(d, core),
                )
            )
        for copy in spread:
            copy.wait_send()
        return sent, swapped

    def gather(s, sent, swapped):
        swapped[0].wait_recv()
        total = own_part[s, 0] + half_recv[s, 0]
        for copy in sent:
            copy.wait_recv()
        for d in near:
            total = total + near_recv[s, d]
        for n in range(CORES):
            total = total + far_recv[s, n]
        mine = piece_at(0, core)
        merged[s, mine] = total
        here = merged.at[s, mine]
        gathered = {
            d: send(here, here, (m_ssem, m_rsem), (s, d), leaf=leaf_at(d, core)) for d in near
        }
        straight = [
            send(here, here, (o_ssem, o_rsem), (s, n), leaf=leaf_at(far, at_core))
            for n, at_core in enumerate((core, other))
        ]
        passed = {0: send(here, here, (p_ssem, p_rsem), (s, 0), leaf=partner)}
        arrived(s, mine)
        for copy in sent + list(swapped.values()):
            copy.wait_send()
        return gathered, straight, passed

    def pass_on(s, gathered, straight, passed):
        for d in near:
            gathered[d].wait_recv()
            at = merged.at[s, piece_at(nx - d, core)]
            passed[d] = send(at, at, (p_ssem, p_rsem), (s, d), leaf=partner)

    def collect(s, gathered, straight, passed):
        for d in near:
            arrived(s, piece_at(nx - d, core))
        for d in [0] + near:
            passed[d].wait_recv()
            arrived(s, piece_at(nx - d, other))
        for copy, at_core in zip(straight, (core, other)):
            copy.wait_recv()
            arrived(s, piece_at(far, at_core))
        for copy in list(gathered.values()) + straight + list(passed.values()):
            copy.wait_send()

    def iterate(k, is_first):
        spreads = []
        for s in streams:
            alpha, beta, _, spread = condense(s, k, is_first)
            spreads.append(spread)
            finish(s, k, alpha, beta, is_first)
        moves = [merge(s, k, spreads[s]) for s in streams]
        moves = [gather(s, *moves[s]) for s in streams]
        pass_on(0, *moves[0])
        collect(0, *moves[0])
        project(0, lambda: pass_on(1, *moves[1]))
        collect(1, *moves[1])
        project(1)
        return 0

    project_first()
    iterate(0, True)
    lax.fori_loop(1, ITERS - 1, lambda k, _: iterate(k, False), 0)

    end = ITERS - 1
    ends = [condense(s, end, False) for s in streams]

    def both_streams(values):
        return select(*(both_sides(value) for value in values))

    own = both_streams([own for _, _, own, _ in ends])
    q_send[...] = own
    q_recv[leaf] = own
    over_leaf = [
        send(
            q_send, q_recv.at[leaf], (q_ssem, q_rsem), d, leaf=(leaf + d) % leaves
        )
        for d in range(1, leaves)
    ]
    totals = []
    for s, (alpha, beta, _, _) in enumerate(ends):
        advance(s, alpha, beta)
        q = jnp.zeros((8, cols), F32)
        for i in range(0, rows // 2, tile):
            new = direction[s, i : i + tile, :]
            q = q + (diag_full[i : i + tile, :] * new * new).reshape(-1, 8, cols).sum(axis=0)
        totals.append(q)
    q = both_streams(totals)
    for copy in over_leaf:
        copy.wait_recv()
    for n in range(leaves):
        q = q + q_recv[n]
    g_send[...] = q
    g_recv[front] = q
    over_front = [
        send(
            g_send,
            g_recv.at[front],
            (g_ssem, g_rsem),
            dz * ny + dy,
            front=front_at(dz, dy),
        )
        for dz, dy in peers
    ]
    for s, (alpha, _, _, _) in enumerate(ends):
        subtract(s, end - 1, alpha)

    def widen(n, _):
        at = pl.ds(pl.multiple_of(n * half_piece, half_piece), half_piece)
        to = pl.ds(pl.multiple_of(n * piece, piece), piece)
        x_out[to, :] = full(x_ref[0, at, :], x_ref[1, at, :])
        direction_out[to, :] = full(direction[0, at, :], direction[1, at, :])
        return 0

    lax.fori_loop(0, rows // piece, widen, 0)

    def widen_interior(n, _):
        at = pl.ds(pl.multiple_of(n * half_rank, half_rank), half_rank)
        to = pl.ds(pl.multiple_of(n * rank, rank), rank)
        interior_out[to, :] = full(interior[0, at, :], interior[1, at, :])
        return 0

    lax.fori_loop(0, fronts, widen_interior, 0)
    for s, (_, _, _, spread) in enumerate(ends):
        for dz, dy in peers:
            projection(s, dz, dy).wait_send()
        for copy in spread:
            copy.wait_recv()
    for n in range(fronts):
        at = slice(n * half_rank, (n + 1) * half_rank)
        last_out[n * rank : (n + 1) * rank, :] = full(c_full[end, 0, at, :], c_full[end, 1, at, :])
    for copy in over_front:
        copy.wait_recv()
    q = g_recv[0]
    for n in range(1, fronts):
        q = q + g_recv[n]
    step_ref[...] = select(rr_ref[0], rr_ref[1]) / q.sum(axis=0, keepdims=True)
    for _, _, _, spread in ends:
        for copy in spread:
            copy.wait_send()
    for copy in over_leaf + over_front:
        copy.wait_send()


def per_device(sources, order, diagonal, coupling, interior_inverse, interior_load, grid=(NZ, NY, NX)):
    nz, ny, nx = grid
    fronts, leaves = nz * ny, nx * CORES
    rows, cols = sources.shape
    depth = coupling.shape[1]
    blocks, rank = interior_inverse.shape[:2]
    assert blocks == fronts and depth == blocks * rank
    piece = rows // 2 // nx
    vmem = pl.BlockSpec(memory_space=pltpu.VMEM)
    dma = pltpu.SemaphoreType.DMA
    field = pltpu.VMEM((rows, cols), F32)
    halves = pltpu.VMEM((STREAMS, rows // 2, cols), F32)
    hbm = pl.BlockSpec(memory_space=pltpu.HBM)
    whole = jax.ShapeDtypeStruct((rows, cols), F32)
    inner = jax.ShapeDtypeStruct((depth, cols), F32)
    x, direction, interior, coeff, step = pl.pallas_call(
        functools.partial(front_solve, grid),
        out_shape=(whole, whole, inner, inner, jax.ShapeDtypeStruct((1, cols), F32)),
        in_specs=[hbm] * 6,
        out_specs=(vmem,) * 5,
        scratch_shapes=[
            pltpu.SMEM((rows,), jnp.int32),
            field,
            pltpu.VMEM((rows // 128, 128), F32),
            pltpu.VMEM(interior_inverse.shape, F32),
            pltpu.VMEM(interior_load.shape, F32),
            pltpu.VMEM((rows, depth), F32),
            pltpu.VMEM((rows, depth), BF16),
            pltpu.VMEM((rows, depth), BF16),
            pltpu.VMEM((depth, rows), BF16),
            pltpu.VMEM((depth, rows), BF16),
            pltpu.VMEM((STREAMS, max(rows, depth), cols), BF16),
            pltpu.VMEM((2 * cols, rows), BF16),
            field,
            halves,
            halves,
            halves,
            halves,
            pltpu.VMEM((STREAMS, depth // 2, cols), F32),
            pltpu.VMEM((rows // 2, cols), F32),
            pltpu.VMEM((STREAMS, fronts, rank // 2 + EXTRA, cols), F32),
            pltpu.VMEM((STREAMS, fronts, rank // 2 + EXTRA, cols), F32),
            pltpu.VMEM((STREAMS, rank // 2, cols), F32),
            pltpu.VMEM((ITERS, STREAMS, depth // 2, cols), F32),
            pltpu.VMEM((STREAMS, nx, piece // 2, cols), F32),
            pltpu.VMEM((STREAMS, nx, piece // 2, cols), F32),
            pltpu.VMEM((STREAMS, CORES, piece // 2, cols), F32),
            pltpu.VMEM((STREAMS, CORES, piece // 2, cols), F32),
            pltpu.VMEM((STREAMS, nx, piece // 2, cols), F32),
            pltpu.VMEM((STREAMS, nx, piece // 2, cols), F32),
            pltpu.VMEM((STREAMS, nx, piece // 2, cols), F32),
            pltpu.VMEM((STREAMS, CORES * nx, piece // 2, cols), F32),
            pltpu.VMEM((STREAMS, CORES * nx, SUMS, 8, cols), F32),
            pltpu.VMEM((STREAMS, rank // 2, cols), F32),
            pltpu.VMEM((STREAMS, rank // 2, cols), F32),
            pltpu.VMEM((STREAMS, 1, cols), F32),
            pltpu.VMEM((8, cols), F32),
            pltpu.VMEM((leaves, 8, cols), F32),
            pltpu.VMEM((8, cols), F32),
            pltpu.VMEM((fronts, 8, cols), F32),
            dma((5,)),
            dma((min(8, rows // 128),)),
            dma((STREAMS, fronts)),
            dma((STREAMS, fronts)),
            dma((STREAMS, fronts)),
            dma((STREAMS, fronts)),
            dma((STREAMS, nx)),
            dma((STREAMS, nx)),
            dma((STREAMS, CORES)),
            dma((STREAMS, CORES)),
            dma((STREAMS, nx)),
            dma((STREAMS, nx)),
            dma((STREAMS, nx)),
            dma((STREAMS, nx)),
            dma((STREAMS, CORES)),
            dma((STREAMS, CORES)),
            dma((STREAMS, nx)),
            dma((STREAMS, nx)),
            dma((leaves,)),
            dma((leaves,)),
            dma((fronts,)),
            dma((fronts,)),
        ],
        compiler_params=pltpu.CompilerParams(
            collective_id=0, has_side_effects=True, vmem_limit_bytes=48 << 20
        ),
        name="front_solve",
    )(
        *(
            pltpu.with_memory_space_constraint(value, pltpu.HBM)
            for value in (
                order,
                sources,
                diagonal.reshape(rows // 128, 128),
                coupling,
                interior_inverse,
                interior_load,
            )
        )
    )
    interior = interior - step * coeff
    return x + step * direction, interior.reshape(interior_load.shape)


def solution(mesh):
    in_specs = (
        P(("wave", "front"), None),
        P("front"),
        P(("wave", "front")),
        P(("wave", "front"), "leaf"),
        P(("wave", "leaf"), None, None),
        P(("wave", "leaf"), None, None),
    )
    out_specs = (P(("wave", "front"), None), P(("wave", "leaf"), None, None))
    return jax.shard_map(
        per_device, mesh=mesh, in_specs=in_specs, out_specs=out_specs, check_vma=False
    )
```

```python
import functools

import jax
import jax.numpy as jnp
from jax import lax
from jax.experimental import pallas as pl
from jax.experimental.pallas import tpu as pltpu
from jax.sharding import PartitionSpec as P

ITERS = 4
NZ, NY, NX, CORES = 4, 4, 4, 2
EXTRA = 8
SUMS = 3
STREAMS = 2
HIGHEST = lax.Precision.HIGHEST
F32 = jnp.float32
BF16 = jnp.bfloat16


def far_first(n):
    return sorted(range(n), key=lambda d: -min(d, n - d))


def split(value):
    high = value.astype(BF16)
    return high, (value - high.astype(F32)).astype(BF16)


def front_solve(
    grid,
    order_hbm,
    sources_hbm,
    diag_hbm,
    coupling_hbm,
    inverse_hbm,
    load_hbm,
    x_out,
    direction_out,
    interior_out,
    last_out,
    step_ref,
    order_ref,
    sources_ref,
    diag_ref,
    inverse_ref,
    load_ref,
    stage,
    c_high,
    c_low,
    t_high,
    t_low,
    rhs,
    turned,
    loads_ref,
    x_ref,
    image,
    residual,
    direction,
    interior,
    diag_full,
    w_send,
    w_recv,
    c_send,
    c_full,
    half_send,
    half_recv,
    far_send,
    far_recv,
    own_part,
    near_send,
    near_recv,
    merged,
    piece_sums,
    tr_ref,
    td_ref,
    rr_ref,
    q_send,
    q_recv,
    g_send,
    g_recv,
    load_sem,
    stage_sem,
    w_ssem,
    w_rsem,
    c_ssem,
    c_rsem,
    h_ssem,
    h_rsem,
    f_ssem,
    f_rsem,
    n_ssem,
    n_rsem,
    m_ssem,
    m_rsem,
    o_ssem,
    o_rsem,
    p_ssem,
    p_rsem,
    q_ssem,
    q_rsem,
    g_ssem,
    g_rsem,
):
    nz, ny, nx = grid
    fronts, leaves = nz * ny, nx * CORES
    rows, cols = loads_ref.shape
    depth = stage.shape[1]
    rank = inverse_ref.shape[1]
    piece = rows // 2 // nx
    tile, lanes = 128, cols // 2
    half_rank, half_piece = rank // 2, piece // 2
    streams = range(STREAMS)
    front = lax.axis_index("front")
    leaf = lax.axis_index("leaf")
    z, y = front // ny, front % ny
    x, core = leaf // CORES, leaf % CORES
    partner, other = x * CORES + (1 - core), 1 - core

    z_steps, y_steps = far_first(nz), far_first(ny)
    far = nx // 2
    near = [d for d in range(1, nx) if d != far]
    peers = [(dz, dy) for dz in z_steps for dy in y_steps if dz or dy]
    peers.sort(key=lambda d: -min(d[0], nz - d[0]) - min(d[1], ny - d[1]))

    chips = [(dx, dz, dy) for dx in far_first(nx) for dz in z_steps for dy in y_steps if dx or dz or dy]
    chips.sort(key=lambda d: -sum(min(i, n - i) for i, n in zip(d, (nx, nz, ny))))

    def front_at(dz, dy):
        return ((z + dz) % nz) * ny + (y + dy) % ny

    def leaf_at(dx, at_core):
        return ((x + dx) % nx) * CORES + at_core

    def piece_at(dx, at_core):
        return at_core * nx + (x + dx) % nx

    def remote(source, target, sems, at, **place):
        return pltpu.make_async_remote_copy(
            src_ref=source,
            dst_ref=target,
            send_sem=sems[0].at[at],
            recv_sem=sems[1].at[at],
            device_id=place,
        )

    def send(*args, **place):
        copy = remote(*args, **place)
        copy.start()
        return copy

    def swap(value):
        return pltpu.roll(value, lanes, 1)

    def select(a, b):
        return jnp.where(lax.broadcasted_iota(jnp.int32, a.shape, 1) < lanes, a, b)

    def packed(value, s):
        top, bottom = jnp.split(value, 2)
        return select(top, swap(bottom)) if s == 0 else select(swap(top), bottom)

    def full(a, b):
        return jnp.concatenate([select(a, swap(b)), select(swap(a), b)])

    def fold(products):
        top, bottom = jnp.split(products + swap(products), 2)
        return select(top, bottom)

    def operand(value):
        high = value.astype(BF16).astype(F32)
        low = value - high
        return jnp.concatenate([select(high, swap(low)), select(swap(high), low)]).astype(BF16)

    def both_sides(row):
        return row + swap(row)

    loads = [
        pltpu.make_async_copy(source, here, load_sem.at[i])
        for i, (source, here) in enumerate(
            (
                (order_hbm, order_ref),
                (sources_hbm, sources_ref),
                (diag_hbm, diag_ref),
                (inverse_hbm, inverse_ref),
                (load_hbm, load_ref),
            )
        )
    ]
    for copy in loads[:2]:
        copy.start()
    stages = []
    step_rows = rows // stage_sem.shape[0]
    for i in range(stage_sem.shape[0]):
        part = pl.ds(i * step_rows, step_rows)
        stages.append(
            pltpu.make_async_copy(coupling_hbm.at[part], stage.at[part], stage_sem.at[i])
        )
        stages[-1].start()
    for copy in loads[2:]:
        copy.start()

    barrier = pltpu.get_barrier_semaphore()
    for dz, dy in peers:
        pl.semaphore_signal(barrier, inc=1, device_id={"front": front_at(dz, dy)})
    for d in range(1, leaves):
        pl.semaphore_signal(barrier, inc=1, device_id={"leaf": (leaf + d) % leaves})
    for dx, dz, dy in chips:
        if dx and (dz or dy):
            pl.semaphore_signal(
                barrier, inc=1, device_id={"leaf": leaf_at(dx, core), "front": front_at(dz, dy)}
            )

    def products(s, n, im, others):
        for i, field in enumerate(others):
            piece_sums[s, n, i] = (field * im).reshape(-1, 8, cols).sum(axis=0)

    for copy in loads[:2]:
        copy.wait()

    for i, copy in enumerate(stages):
        copy.wait()

        def prepare(j, _, i=i):
            first = i * step_rows + j * 16
            at = pl.ds(pl.multiple_of(first, 16), 16)
            high, low = split(stage[at, :])
            c_high[at, :] = high
            c_low[at, :] = low
            for n in range(16):
                row = pl.ds(order_ref[first + n] & (rows - 1), 1)
                loads_ref[pl.ds(first + n, 1), :] = sources_ref[row, :]
            return 0

        lax.fori_loop(0, step_rows // 16, prepare, 0)
    square = jnp.zeros((8, cols), F32)
    for i in range(0, rows, tile):
        high, low = split(loads_ref[i : i + tile, :].T)
        turned[0:cols, i : i + tile] = high
        turned[cols:, i : i + tile] = low
        block = loads_ref[i : i + tile, :]
        square = square + (block * block).reshape(-1, 8, cols).sum(axis=0)
    square = square.sum(axis=0, keepdims=True)

    def start_fields(n, _):
        block = loads_ref[pl.ds(pl.multiple_of(n * piece, piece), piece), :]
        at = pl.ds(pl.multiple_of(n * half_piece, half_piece), half_piece)
        for s in streams:
            value = packed(block, s)
            image[s, at, :] = value
            residual[s, at, :] = value
            direction[s, at, :] = value
            x_ref[s, at, :] = jnp.zeros_like(value)
        return 0

    def turn(start, stop):
        def columns(j, _):
            for r in range(start, stop, tile):
                at = pl.ds(pl.multiple_of(j * tile, tile), tile)
                high, low = split(stage[r : r + tile, at].T)
                t_high[at, r : r + tile] = high
                t_low[at, r : r + tile] = low
            return 0

        lax.fori_loop(0, depth // tile, columns, 0)

    def spread_diagonal():
        for n in range(rows // piece):
            first = n * piece
            row = diag_ref[first // tile : first // tile + 1, first % tile : first % tile + piece]
            column = jnp.broadcast_to(row, (tile, piece)).T
            at = slice(n * half_piece, (n + 1) * half_piece)
            diag_full[at, :] = select(column[:half_piece], column[half_piece:])

    def start_interior():
        for n in range(fronts):
            value = jnp.dot(
                inverse_ref[n], load_ref[n], precision=HIGHEST, preferred_element_type=F32
            )
            for s in streams:
                interior[s, n * half_rank : (n + 1) * half_rank, :] = packed(value, s)

    pl.semaphore_wait(barrier, len(peers) + leaves - 1 + (nx - 1) * len(peers))

    def times(high_ref, low_ref, s, starts, size):
        unit = size // 2
        units = [pl.ds(pl.multiple_of(at + i, unit), unit) for at in starts for i in (0, unit)]
        both = []
        for part in (units[: len(starts)], units[len(starts) :]):
            high = jnp.concatenate([high_ref[at, :] for at in part])
            low = jnp.concatenate([low_ref[at, :] for at in part])
            out = jnp.dot(high, rhs[s], preferred_element_type=F32)
            both.append(out + jnp.dot(low, rhs[s], preferred_element_type=F32))
        return jnp.concatenate(both)

    def times_turned():
        n = depth // 2
        both = []
        for i in (0, n):
            at = slice(i, i + n)
            out = jnp.dot(turned[...], c_high[:, at], preferred_element_type=F32)
            both.append(out + jnp.dot(turned[...], c_low[:, at], preferred_element_type=F32))
        both = [out[:cols] + out[cols:] for out in both]
        return jnp.concatenate([out[:, i : i + tile].T for out in both for i in range(0, n, tile)])

    def arrived(s, n):
        at = pl.ds(pl.multiple_of(n * half_piece, half_piece), half_piece)
        along = direction[s, at, :]
        new = diag_full[at, :] * along + merged[s, n]
        image[s, at, :] = new
        rhs[s, pl.ds(pl.multiple_of(n * piece, piece), piece), :] = operand(new)
        products(s, n, new, (along, residual[s, at, :], new))

    size = half_rank + SUMS

    def projection(s, dz, dy):
        to = front_at(dz, dy)
        return remote(
            w_send.at[s, to, 0:size],
            w_recv.at[s, front, 0:size],
            (w_ssem, w_rsem),
            (s, dz * ny + dy),
            front=to,
        )

    def sums_of(s):
        sums = [piece_sums[s, 0, n] for n in range(SUMS)]
        for i in range(1, rows // piece):
            sums = [total + piece_sums[s, i, n] for n, total in enumerate(sums)]
        sums = [both_sides(total.sum(axis=0, keepdims=True)) for total in sums]
        return jnp.concatenate(sums + [jnp.zeros((EXTRA - SUMS, cols), F32)])

    def project_first():
        out = times_turned()
        for s in streams:
            norm = select(square, swap(square)) if s == 0 else select(swap(square), square)
            dots = jnp.concatenate([norm] * SUMS + [jnp.zeros((EXTRA - SUMS, cols), F32)])
            for j in range(fronts):
                w_send[s, j, 0:half_rank, :] = packed(out[j * rank : (j + 1) * rank], s)
                w_send[s, j, half_rank:, :] = dots
            for dz, dy in peers:
                projection(s, dz, dy).start()
        lax.fori_loop(0, rows // piece, start_fields, 0)

    def project(s, between=None):
        dots = sums_of(s)
        span = ny * rank
        for i in range(0, nz, 2):
            steps = z_steps[i : i + 2]
            places = [(z + dz) % nz for dz in steps]
            out = times(t_high, t_low, s, [p * span for p in places], span)
            for n, place in enumerate(places):
                for j in range(ny):
                    at = n * span + j * rank
                    w_send[s, place * ny + j, 0:half_rank, :] = fold(out[at : at + rank])
                    w_send[s, place * ny + j, half_rank:, :] = dots
            for dz, dy in peers:
                if dz in steps:
                    projection(s, dz, dy).start()
            if between and i:
                between()

    def condense(s, k, is_first):
        w_recv[s, front, 0:size, :] = w_send[s, front, 0:size, :]
        if is_first and s == 0:
            turn(0, rows // 2)
            loads[3].wait()
        for dz, dy in peers:
            projection(s, dz, dy).wait_recv()
        total = w_recv[s, 0]
        for n in range(1, fronts):
            total = total + w_recv[s, n]
        w = total[0:half_rank]
        curvature, cross, square = (total[half_rank + n : half_rank + n + 1] for n in range(SUMS))
        if is_first:
            alpha = beta = None
            rr_ref[s] = square
            tr = td = w
        else:
            rr = rr_ref[s]
            alpha = rr / curvature
            rr_next = rr - 2.0 * alpha * cross + alpha * alpha * square
            beta = rr_next / rr
            rr_ref[s] = rr_next
            tr = tr_ref[s] - alpha * w
            td = tr + beta * td_ref[s]
        tr_ref[s] = tr
        td_ref[s] = td
        coeff = jnp.dot(
            inverse_ref[front],
            jnp.concatenate([td, swap(td)]),
            precision=HIGHEST,
            preferred_element_type=F32,
        )
        coeff = packed(coeff, 0)
        here = pl.ds(pl.multiple_of(front * half_rank, half_rank), half_rank)
        c_send[s] = coeff
        c_full[k, s, here, :] = coeff
        spread = [
            send(
                c_send.at[s],
                c_full.at[k, s, here],
                (c_ssem, c_rsem),
                (s, dz * ny + dy),
                front=front_at(dz, dy),
            )
            for dz, dy in peers
        ]
        return alpha, beta, (td * coeff).reshape(-1, 8, cols).sum(axis=0), spread

    def advance(s, alpha, beta):
        for i in range(0, rows // 2, tile):
            at = slice(i, i + tile)
            x_ref[s, at, :] += alpha * direction[s, at, :]
            res = residual[s, at, :] - alpha * image[s, at, :]
            residual[s, at, :] = res
            direction[s, at, :] = res + beta * direction[s, at, :]

    def subtract(s, k, step):
        for i in range(0, depth // 2, tile):
            at = slice(i, i + tile)
            interior[s, at, :] = interior[s, at, :] - step * c_full[k, s, at, :]

    def finish(s, k, alpha, beta, is_first):
        if not is_first:
            advance(s, alpha, beta)
            subtract(s, k - 1, alpha)
        elif s == 0:
            for copy in (loads[2], loads[4]):
                copy.wait()
            turn(rows // 2, rows)
        else:
            spread_diagonal()
            start_interior()
        for dz, dy in peers:
            projection(s, dz, dy).wait_send()

    def merge(s, k, spread):
        for copy in spread:
            copy.wait_recv()
        for n in range(fronts):
            rhs[s, n * rank : (n + 1) * rank, :] = operand(
                c_full[k, s, n * half_rank : (n + 1) * half_rank, :]
            )

        def field(pieces):
            out = times(c_high, c_low, s, [n * piece for n in pieces], piece)
            return [fold(out[i * piece : (i + 1) * piece]) for i in range(len(pieces))]

        def swap_over(d):
            return send(
                half_send.at[s, d], half_recv.at[s, d], (h_ssem, h_rsem), (s, d), leaf=partner
            )

        swapped = {}
        if near:
            for d, value in zip(near, field([piece_at(d, other) for d in near])):
                half_send[s, d] = value
            for d in near:
                swapped[d] = swap_over(d)
        sent = []
        ends = (other, core)
        for at_core, value in zip(ends, field([piece_at(far, n) for n in ends])):
            far_send[s, at_core] = value
        for n, at_core in enumerate(ends):
            sent.append(
                send(
                    far_send.at[s, at_core],
                    far_recv.at[s, core],
                    (f_ssem, f_rsem),
                    (s, 1 - n),
                    leaf=leaf_at(far, at_core),
                )
            )
        steps = near + [0]
        values = field([piece_at(0, other)] + [piece_at(d, core) for d in steps])
        half_send[s, 0] = values[0]
        swapped[0] = swap_over(0)
        for d, value in zip(steps, values[1:]):
            own_part[s, d] = value
        for d in near:
            swapped[d].wait_recv()
            near_send[s, d] = own_part[s, d] + half_recv[s, d]
            sent.append(
                send(
                    near_send.at[s, d],
                    near_recv.at[s, d],
                    (n_ssem, n_rsem),
                    (s, d),
                    leaf=leaf_at(d, core),
                )
            )
        for copy in spread:
            copy.wait_send()
        return sent, swapped

    def gather(s, sent, swapped):
        swapped[0].wait_recv()
        total = own_part[s, 0] + half_recv[s, 0]
        for copy in sent:
            copy.wait_recv()
        for d in near:
            total = total + near_recv[s, d]
        for n in range(CORES):
            total = total + far_recv[s, n]
        mine = piece_at(0, core)
        merged[s, mine] = total
        here = merged.at[s, mine]
        gathered = {
            d: send(here, here, (m_ssem, m_rsem), (s, d), leaf=leaf_at(d, core)) for d in near
        }
        straight = [
            send(here, here, (o_ssem, o_rsem), (s, n), leaf=leaf_at(far, at_core))
            for n, at_core in enumerate((core, other))
        ]
        passed = {0: send(here, here, (p_ssem, p_rsem), (s, 0), leaf=partner)}
        arrived(s, mine)
        for copy in sent + list(swapped.values()):
            copy.wait_send()
        return gathered, straight, passed

    def pass_on(s, gathered, straight, passed):
        for d in near:
            gathered[d].wait_recv()
            at = merged.at[s, piece_at(nx - d, core)]
            passed[d] = send(at, at, (p_ssem, p_rsem), (s, d), leaf=partner)

    def collect(s, gathered, straight, passed):
        for d in near:
            arrived(s, piece_at(nx - d, core))
        for d in [0] + near:
            passed[d].wait_recv()
            arrived(s, piece_at(nx - d, other))
        for copy, at_core in zip(straight, (core, other)):
            copy.wait_recv()
            arrived(s, piece_at(far, at_core))
        for copy in list(gathered.values()) + straight + list(passed.values()):
            copy.wait_send()

    def iterate(k, is_first):
        spreads = []
        for s in streams:
            alpha, beta, _, spread = condense(s, k, is_first)
            spreads.append(spread)
            finish(s, k, alpha, beta, is_first)
        moves = [merge(s, k, spreads[s]) for s in streams]
        moves = [gather(s, *moves[s]) for s in streams]
        pass_on(0, *moves[0])
        collect(0, *moves[0])
        project(0, lambda: pass_on(1, *moves[1]))
        collect(1, *moves[1])
        project(1)
        return 0

    project_first()
    iterate(0, True)
    lax.fori_loop(1, ITERS - 1, lambda k, _: iterate(k, False), 0)

    end = ITERS - 1
    ends = [condense(s, end, False) for s in streams]

    def both_streams(values):
        return select(*(both_sides(value) for value in values))

    own = both_streams([own for _, _, own, _ in ends]).sum(axis=0, keepdims=True)
    q_send[0:1, :] = own
    over_chip = send(
        q_send.at[0:1], q_recv.at[0:1], (q_ssem, q_rsem), 0, leaf=partner
    )
    totals = []
    for s, (alpha, beta, _, _) in enumerate(ends):
        advance(s, alpha, beta)
        q = jnp.zeros((8, cols), F32)
        for i in range(0, rows // 2, tile):
            new = direction[s, i : i + tile, :]
            q = q + (diag_full[i : i + tile, :] * new * new).reshape(-1, 8, cols).sum(axis=0)
        totals.append(q)
    q = both_streams(totals).sum(axis=0, keepdims=True) * (1.0 / nx)
    over_chip.wait_recv()
    q = q + (own + q_recv[0:1, :])
    g_send[0:1, :] = q
    place = x * fronts + front
    g_recv[place, 0:1, :] = q
    over_all = [
        send(
            g_send.at[0:1],
            g_recv.at[place, 0:1],
            (g_ssem, g_rsem),
            (dx * nz + dz) * ny + dy,
            leaf=leaf_at(dx, core),
            front=front_at(dz, dy),
        )
        for dx, dz, dy in chips
    ]
    for s, (alpha, _, _, _) in enumerate(ends):
        subtract(s, end - 1, alpha)

    def widen(n, _):
        at = pl.ds(pl.multiple_of(n * half_piece, half_piece), half_piece)
        to = pl.ds(pl.multiple_of(n * piece, piece), piece)
        x_out[to, :] = full(x_ref[0, at, :], x_ref[1, at, :])
        direction_out[to, :] = full(direction[0, at, :], direction[1, at, :])
        return 0

    lax.fori_loop(0, rows // piece, widen, 0)

    def widen_interior(n, _):
        at = pl.ds(pl.multiple_of(n * half_rank, half_rank), half_rank)
        to = pl.ds(pl.multiple_of(n * rank, rank), rank)
        interior_out[to, :] = full(interior[0, at, :], interior[1, at, :])
        return 0

    lax.fori_loop(0, fronts, widen_interior, 0)
    for s, (_, _, _, spread) in enumerate(ends):
        for dz, dy in peers:
            projection(s, dz, dy).wait_send()
        for copy in spread:
            copy.wait_recv()
    for n in range(fronts):
        at = slice(n * half_rank, (n + 1) * half_rank)
        last_out[n * rank : (n + 1) * rank, :] = full(c_full[end, 0, at, :], c_full[end, 1, at, :])
    for copy in over_all:
        copy.wait_recv()
    q = g_recv[0, 0:1, :]
    for n in range(1, nx * fronts):
        q = q + g_recv[n, 0:1, :]
    step_ref[...] = select(rr_ref[0], rr_ref[1]) / q
    for _, _, _, spread in ends:
        for copy in spread:
            copy.wait_send()
    for copy in [over_chip] + over_all:
        copy.wait_send()


def per_device(sources, order, diagonal, coupling, interior_inverse, interior_load, grid=(NZ, NY, NX)):
    nz, ny, nx = grid
    fronts, leaves = nz * ny, nx * CORES
    rows, cols = sources.shape
    depth = coupling.shape[1]
    blocks, rank = interior_inverse.shape[:2]
    assert blocks == fronts and depth == blocks * rank
    piece = rows // 2 // nx
    vmem = pl.BlockSpec(memory_space=pltpu.VMEM)
    dma = pltpu.SemaphoreType.DMA
    field = pltpu.VMEM((rows, cols), F32)
    halves = pltpu.VMEM((STREAMS, rows // 2, cols), F32)
    hbm = pl.BlockSpec(memory_space=pltpu.HBM)
    whole = jax.ShapeDtypeStruct((rows, cols), F32)
    inner = jax.ShapeDtypeStruct((depth, cols), F32)
    x, direction, interior, coeff, step = pl.pallas_call(
        functools.partial(front_solve, grid),
        out_shape=(whole, whole, inner, inner, jax.ShapeDtypeStruct((1, cols), F32)),
        in_specs=[hbm] * 6,
        out_specs=(vmem,) * 5,
        scratch_shapes=[
            pltpu.SMEM((rows,), jnp.int32),
            field,
            pltpu.VMEM((rows // 128, 128), F32),
            pltpu.VMEM(interior_inverse.shape, F32),
            pltpu.VMEM(interior_load.shape, F32),
            pltpu.VMEM((rows, depth), F32),
            pltpu.VMEM((rows, depth), BF16),
            pltpu.VMEM((rows, depth), BF16),
            pltpu.VMEM((depth, rows), BF16),
            pltpu.VMEM((depth, rows), BF16),
            pltpu.VMEM((STREAMS, max(rows, depth), cols), BF16),
            pltpu.VMEM((2 * cols, rows), BF16),
            field,
            halves,
            halves,
            halves,
            halves,
            pltpu.VMEM((STREAMS, depth // 2, cols), F32),
            pltpu.VMEM((rows // 2, cols), F32),
            pltpu.VMEM((STREAMS, fronts, rank // 2 + EXTRA, cols), F32),
            pltpu.VMEM((STREAMS, fronts, rank // 2 + EXTRA, cols), F32),
            pltpu.VMEM((STREAMS, rank // 2, cols), F32),
            pltpu.VMEM((ITERS, STREAMS, depth // 2, cols), F32),
            pltpu.VMEM((STREAMS, nx, piece // 2, cols), F32),
            pltpu.VMEM((STREAMS, nx, piece // 2, cols), F32),
            pltpu.VMEM((STREAMS, CORES, piece // 2, cols), F32),
            pltpu.VMEM((STREAMS, CORES, piece // 2, cols), F32),
            pltpu.VMEM((STREAMS, nx, piece // 2, cols), F32),
            pltpu.VMEM((STREAMS, nx, piece // 2, cols), F32),
            pltpu.VMEM((STREAMS, nx, piece // 2, cols), F32),
            pltpu.VMEM((STREAMS, CORES * nx, piece // 2, cols), F32),
            pltpu.VMEM((STREAMS, CORES * nx, SUMS, 8, cols), F32),
            pltpu.VMEM((STREAMS, rank // 2, cols), F32),
            pltpu.VMEM((STREAMS, rank // 2, cols), F32),
            pltpu.VMEM((STREAMS, 1, cols), F32),
            pltpu.VMEM((8, cols), F32),
            pltpu.VMEM((8, cols), F32),
            pltpu.VMEM((8, cols), F32),
            pltpu.VMEM((nx * fronts, 8, cols), F32),
            dma((5,)),
            dma((min(8, rows // 128),)),
            dma((STREAMS, fronts)),
            dma((STREAMS, fronts)),
            dma((STREAMS, fronts)),
            dma((STREAMS, fronts)),
            dma((STREAMS, nx)),
            dma((STREAMS, nx)),
            dma((STREAMS, CORES)),
            dma((STREAMS, CORES)),
            dma((STREAMS, nx)),
            dma((STREAMS, nx)),
            dma((STREAMS, nx)),
            dma((STREAMS, nx)),
            dma((STREAMS, CORES)),
            dma((STREAMS, CORES)),
            dma((STREAMS, nx)),
            dma((STREAMS, nx)),
            dma((1,)),
            dma((1,)),
            dma((nx * fronts,)),
            dma((nx * fronts,)),
        ],
        compiler_params=pltpu.CompilerParams(
            collective_id=0, has_side_effects=True, vmem_limit_bytes=48 << 20
        ),
        name="front_solve",
    )(
        *(
            pltpu.with_memory_space_constraint(value, pltpu.HBM)
            for value in (
                order,
                sources,
                diagonal.reshape(rows // 128, 128),
                coupling,
                interior_inverse,
                interior_load,
            )
        )
    )
    interior = interior - step * coeff
    return x + step * direction, interior.reshape(interior_load.shape)


def solution(mesh):
    in_specs = (
        P(("wave", "front"), None),
        P("front"),
        P(("wave", "front")),
        P(("wave", "front"), "leaf"),
        P(("wave", "leaf"), None, None),
        P(("wave", "leaf"), None, None),
    )
    out_specs = (P(("wave", "front"), None), P(("wave", "leaf"), None, None))
    return jax.shard_map(
        per_device, mesh=mesh, in_specs=in_specs, out_specs=out_specs, check_vma=False
    )
```

```python
import functools

import jax
import jax.numpy as jnp
from jax import lax
from jax.experimental import pallas as pl
from jax.experimental.pallas import tpu as pltpu
from jax.sharding import PartitionSpec as P

ITERS = 4
NZ, NY, NX, CORES = 4, 4, 4, 2
EXTRA = 8
SUMS = 3
STREAMS = 2
HIGHEST = lax.Precision.HIGHEST
F32 = jnp.float32
BF16 = jnp.bfloat16


def far_first(n):
    return sorted(range(n), key=lambda d: -min(d, n - d))


def split(value):
    high = value.astype(BF16)
    return high, (value - high.astype(F32)).astype(BF16)


def front_solve(
    grid,
    order_hbm,
    sources_hbm,
    diag_hbm,
    coupling_hbm,
    inverse_hbm,
    load_hbm,
    x_out,
    direction_out,
    interior_out,
    last_out,
    step_ref,
    order_ref,
    sources_ref,
    diag_ref,
    inverse_ref,
    load_ref,
    stage,
    c_high,
    c_low,
    t_high,
    t_low,
    rhs,
    turned,
    loads_ref,
    x_ref,
    image,
    residual,
    direction,
    interior,
    diag_full,
    w_send,
    w_recv,
    c_send,
    c_full,
    half_send,
    half_recv,
    far_send,
    far_recv,
    own_part,
    near_send,
    near_recv,
    merged,
    piece_sums,
    tr_ref,
    td_ref,
    rr_ref,
    q_send,
    q_recv,
    g_send,
    g_recv,
    load_sem,
    stage_sem,
    w_ssem,
    w_rsem,
    c_ssem,
    c_rsem,
    h_ssem,
    h_rsem,
    f_ssem,
    f_rsem,
    n_ssem,
    n_rsem,
    m_ssem,
    m_rsem,
    o_ssem,
    o_rsem,
    p_ssem,
    p_rsem,
    q_ssem,
    q_rsem,
    g_ssem,
    g_rsem,
):
    nz, ny, nx = grid
    fronts, leaves = nz * ny, nx * CORES
    rows, cols = loads_ref.shape
    depth = stage.shape[1]
    rank = inverse_ref.shape[1]
    piece = rows // 2 // nx
    tile, lanes = 128, cols // 2
    half_rank, half_piece = rank // 2, piece // 2
    streams = range(STREAMS)
    front = lax.axis_index("front")
    leaf = lax.axis_index("leaf")
    z, y = front // ny, front % ny
    x, core = leaf // CORES, leaf % CORES
    partner, other = x * CORES + (1 - core), 1 - core

    z_steps, y_steps = far_first(nz), far_first(ny)
    far = nx // 2
    near = [d for d in range(1, nx) if d != far]
    peers = [(dz, dy) for dz in z_steps for dy in y_steps if dz or dy]
    peers.sort(key=lambda d: -min(d[0], nz - d[0]) - min(d[1], ny - d[1]))

    chips = [(dx, dz, dy) for dx in far_first(nx) for dz in z_steps for dy in y_steps if dx or dz or dy]
    chips.sort(key=lambda d: -sum(min(i, n - i) for i, n in zip(d, (nx, nz, ny))))

    def front_at(dz, dy):
        return ((z + dz) % nz) * ny + (y + dy) % ny

    def leaf_at(dx, at_core):
        return ((x + dx) % nx) * CORES + at_core

    def piece_at(dx, at_core):
        return at_core * nx + (x + dx) % nx

    def remote(source, target, sems, at, **place):
        return pltpu.make_async_remote_copy(
            src_ref=source,
            dst_ref=target,
            send_sem=sems[0].at[at],
            recv_sem=sems[1].at[at],
            device_id=place,
        )

    def send(*args, **place):
        copy = remote(*args, **place)
        copy.start()
        return copy

    def swap(value):
        return pltpu.roll(value, lanes, 1)

    def select(a, b):
        return jnp.where(lax.broadcasted_iota(jnp.int32, a.shape, 1) < lanes, a, b)

    def packed(value, s):
        top, bottom = jnp.split(value, 2)
        return select(top, swap(bottom)) if s == 0 else select(swap(top), bottom)

    def full(a, b):
        return jnp.concatenate([select(a, swap(b)), select(swap(a), b)])

    def fold(products):
        top, bottom = jnp.split(products + swap(products), 2)
        return select(top, bottom)

    def operand(value):
        high = value.astype(BF16).astype(F32)
        low = value - high
        return jnp.concatenate([select(high, swap(low)), select(swap(high), low)]).astype(BF16)

    def both_sides(row):
        return row + swap(row)

    loads = [
        pltpu.make_async_copy(source, here, load_sem.at[i])
        for i, (source, here) in enumerate(
            (
                (order_hbm, order_ref),
                (sources_hbm, sources_ref),
                (diag_hbm, diag_ref),
                (inverse_hbm, inverse_ref),
                (load_hbm, load_ref),
            )
        )
    ]
    for copy in loads[:2]:
        copy.start()
    stages = []
    step_rows = rows // stage_sem.shape[0]
    for i in range(stage_sem.shape[0]):
        part = pl.ds(i * step_rows, step_rows)
        stages.append(
            pltpu.make_async_copy(coupling_hbm.at[part], stage.at[part], stage_sem.at[i])
        )
        stages[-1].start()
    for copy in loads[2:]:
        copy.start()

    barrier = pltpu.get_barrier_semaphore()
    for dz, dy in peers:
        pl.semaphore_signal(barrier, inc=1, device_id={"front": front_at(dz, dy)})
    for d in range(1, leaves):
        pl.semaphore_signal(barrier, inc=1, device_id={"leaf": (leaf + d) % leaves})
    for dx, dz, dy in chips:
        if dx and (dz or dy):
            pl.semaphore_signal(
                barrier, inc=1, device_id={"leaf": leaf_at(dx, core), "front": front_at(dz, dy)}
            )

    def products(s, n, im, others):
        for i, field in enumerate(others):
            piece_sums[s, n, i] = (field * im).reshape(-1, 8, cols).sum(axis=0)

    for copy in loads[:2]:
        copy.wait()

    for i, copy in enumerate(stages):
        copy.wait()

        def prepare(j, _, i=i):
            first = i * step_rows + j * 16
            at = pl.ds(pl.multiple_of(first, 16), 16)
            high, low = split(stage[at, :])
            c_high[at, :] = high
            c_low[at, :] = low
            for n in range(16):
                row = pl.ds(order_ref[first + n] & (rows - 1), 1)
                loads_ref[pl.ds(first + n, 1), :] = sources_ref[row, :]
            return 0

        lax.fori_loop(0, step_rows // 16, prepare, 0)
    square = jnp.zeros((8, cols), F32)
    for i in range(0, rows, tile):
        high, low = split(loads_ref[i : i + tile, :].T)
        turned[0:cols, i : i + tile] = high
        turned[cols:, i : i + tile] = low
        block = loads_ref[i : i + tile, :]
        square = square + (block * block).reshape(-1, 8, cols).sum(axis=0)
    square = square.sum(axis=0, keepdims=True)

    def start_fields(n, _):
        block = loads_ref[pl.ds(pl.multiple_of(n * piece, piece), piece), :]
        at = pl.ds(pl.multiple_of(n * half_piece, half_piece), half_piece)
        for s in streams:
            value = packed(block, s)
            image[s, at, :] = value
            residual[s, at, :] = value
            direction[s, at, :] = value
            x_ref[s, at, :] = jnp.zeros_like(value)
        return 0

    def turn(start, stop):
        def columns(j, _):
            for r in range(start, stop, tile):
                at = pl.ds(pl.multiple_of(j * tile, tile), tile)
                high, low = split(stage[r : r + tile, at].T)
                t_high[at, r : r + tile] = high
                t_low[at, r : r + tile] = low
            return 0

        lax.fori_loop(0, depth // tile, columns, 0)

    def spread_diagonal():
        for n in range(rows // piece):
            first = n * piece
            row = diag_ref[first // tile : first // tile + 1, first % tile : first % tile + piece]
            column = jnp.broadcast_to(row, (tile, piece)).T
            at = slice(n * half_piece, (n + 1) * half_piece)
            diag_full[at, :] = select(column[:half_piece], column[half_piece:])

    def start_interior():
        for n in range(fronts):
            value = jnp.dot(
                inverse_ref[n], load_ref[n], precision=HIGHEST, preferred_element_type=F32
            )
            for s in streams:
                interior[s, n * half_rank : (n + 1) * half_rank, :] = packed(value, s)

    pl.semaphore_wait(barrier, len(peers) + leaves - 1 + (nx - 1) * len(peers))

    def times(high_ref, low_ref, s, starts, size):
        unit = size // 2
        units = [pl.ds(pl.multiple_of(at + i, unit), unit) for at in starts for i in (0, unit)]
        both = []
        for part in (units[: len(starts)], units[len(starts) :]):
            high = jnp.concatenate([high_ref[at, :] for at in part])
            low = jnp.concatenate([low_ref[at, :] for at in part])
            out = jnp.dot(high, rhs[s], preferred_element_type=F32)
            both.append(out + jnp.dot(low, rhs[s], preferred_element_type=F32))
        return jnp.concatenate(both)

    def times_turned():
        n = depth // 2
        both = []
        for i in (0, n):
            at = slice(i, i + n)
            out = jnp.dot(turned[...], c_high[:, at], preferred_element_type=F32)
            both.append(out + jnp.dot(turned[...], c_low[:, at], preferred_element_type=F32))
        both = [out[:cols] + out[cols:] for out in both]
        return jnp.concatenate([out[:, i : i + tile].T for out in both for i in range(0, n, tile)])

    def arrived(s, n):
        at = pl.ds(pl.multiple_of(n * half_piece, half_piece), half_piece)
        along = direction[s, at, :]
        new = diag_full[at, :] * along + merged[s, n]
        image[s, at, :] = new
        rhs[s, pl.ds(pl.multiple_of(n * piece, piece), piece), :] = operand(new)
        products(s, n, new, (along, residual[s, at, :], new))

    size = half_rank + SUMS

    def projection(s, dz, dy):
        to = front_at(dz, dy)
        return remote(
            w_send.at[s, to, 0:size],
            w_recv.at[s, front, 0:size],
            (w_ssem, w_rsem),
            (s, dz * ny + dy),
            front=to,
        )

    def sums_of(s):
        sums = [piece_sums[s, 0, n] for n in range(SUMS)]
        for i in range(1, rows // piece):
            sums = [total + piece_sums[s, i, n] for n, total in enumerate(sums)]
        sums = [both_sides(total.sum(axis=0, keepdims=True)) for total in sums]
        return jnp.concatenate(sums + [jnp.zeros((EXTRA - SUMS, cols), F32)])

    def project_first():
        out = times_turned()
        for s in streams:
            norm = select(square, swap(square)) if s == 0 else select(swap(square), square)
            dots = jnp.concatenate([norm] * SUMS + [jnp.zeros((EXTRA - SUMS, cols), F32)])
            for j in range(fronts):
                w_send[s, j, 0:half_rank, :] = packed(out[j * rank : (j + 1) * rank], s)
                w_send[s, j, half_rank:, :] = dots
            for dz, dy in peers:
                projection(s, dz, dy).start()
        lax.fori_loop(0, rows // piece, start_fields, 0)

    def project(s, between=None):
        dots = sums_of(s)
        span = ny * rank
        for i in range(0, nz, 2):
            steps = z_steps[i : i + 2]
            places = [(z + dz) % nz for dz in steps]
            out = times(t_high, t_low, s, [p * span for p in places], span)
            for n, place in enumerate(places):
                for j in range(ny):
                    at = n * span + j * rank
                    w_send[s, place * ny + j, 0:half_rank, :] = fold(out[at : at + rank])
                    w_send[s, place * ny + j, half_rank:, :] = dots
            for dz, dy in peers:
                if dz in steps:
                    projection(s, dz, dy).start()
            if between and i:
                between()

    def condense(s, k, is_first):
        w_recv[s, front, 0:size, :] = w_send[s, front, 0:size, :]
        if is_first and s == 0:
            turn(0, rows // 2)
            loads[3].wait()
        for dz, dy in peers:
            projection(s, dz, dy).wait_recv()
        total = w_recv[s, 0]
        for n in range(1, fronts):
            total = total + w_recv[s, n]
        w = total[0:half_rank]
        curvature, cross, square = (total[half_rank + n : half_rank + n + 1] for n in range(SUMS))
        if is_first:
            alpha = beta = None
            rr_ref[s] = square
            tr = td = w
        else:
            rr = rr_ref[s]
            alpha = rr / curvature
            rr_next = rr - 2.0 * alpha * cross + alpha * alpha * square
            beta = rr_next / rr
            rr_ref[s] = rr_next
            tr = tr_ref[s] - alpha * w
            td = tr + beta * td_ref[s]
        tr_ref[s] = tr
        td_ref[s] = td
        high, low = split(inverse_ref[front])
        right = operand(td)
        coeff = jnp.dot(high, right, preferred_element_type=F32)
        coeff = fold(coeff + jnp.dot(low, right, preferred_element_type=F32))
        here = pl.ds(pl.multiple_of(front * half_rank, half_rank), half_rank)
        c_send[s] = coeff
        c_full[k, s, here, :] = coeff
        spread = [
            send(
                c_send.at[s],
                c_full.at[k, s, here],
                (c_ssem, c_rsem),
                (s, dz * ny + dy),
                front=front_at(dz, dy),
            )
            for dz, dy in peers
        ]
        return alpha, beta, (td * coeff).reshape(-1, 8, cols).sum(axis=0), spread

    def advance(s, alpha, beta):
        for i in range(0, rows // 2, tile):
            at = slice(i, i + tile)
            x_ref[s, at, :] += alpha * direction[s, at, :]
            res = residual[s, at, :] - alpha * image[s, at, :]
            residual[s, at, :] = res
            direction[s, at, :] = res + beta * direction[s, at, :]

    def subtract(s, k, step):
        for i in range(0, depth // 2, tile):
            at = slice(i, i + tile)
            interior[s, at, :] = interior[s, at, :] - step * c_full[k, s, at, :]

    def finish(s, k, alpha, beta, is_first):
        if not is_first:
            advance(s, alpha, beta)
            subtract(s, k - 1, alpha)
        elif s == 0:
            for copy in (loads[2], loads[4]):
                copy.wait()
            turn(rows // 2, rows)
        else:
            spread_diagonal()
            start_interior()
        for dz, dy in peers:
            projection(s, dz, dy).wait_send()

    def merge(s, k, spread):
        for copy in spread:
            copy.wait_recv()
        for n in range(fronts):
            rhs[s, n * rank : (n + 1) * rank, :] = operand(
                c_full[k, s, n * half_rank : (n + 1) * half_rank, :]
            )

        def field(pieces):
            out = times(c_high, c_low, s, [n * piece for n in pieces], piece)
            return [fold(out[i * piece : (i + 1) * piece]) for i in range(len(pieces))]

        def swap_over(d):
            return send(
                half_send.at[s, d], half_recv.at[s, d], (h_ssem, h_rsem), (s, d), leaf=partner
            )

        swapped = {}
        if near:
            for d, value in zip(near, field([piece_at(d, other) for d in near])):
                half_send[s, d] = value
            for d in near:
                swapped[d] = swap_over(d)
        sent = []
        ends = (other, core)
        for at_core, value in zip(ends, field([piece_at(far, n) for n in ends])):
            far_send[s, at_core] = value
        for n, at_core in enumerate(ends):
            sent.append(
                send(
                    far_send.at[s, at_core],
                    far_recv.at[s, core],
                    (f_ssem, f_rsem),
                    (s, 1 - n),
                    leaf=leaf_at(far, at_core),
                )
            )
        steps = near + [0]
        values = field([piece_at(0, other)] + [piece_at(d, core) for d in steps])
        half_send[s, 0] = values[0]
        swapped[0] = swap_over(0)
        for d, value in zip(steps, values[1:]):
            own_part[s, d] = value
        for d in near:
            swapped[d].wait_recv()
            near_send[s, d] = own_part[s, d] + half_recv[s, d]
            sent.append(
                send(
                    near_send.at[s, d],
                    near_recv.at[s, d],
                    (n_ssem, n_rsem),
                    (s, d),
                    leaf=leaf_at(d, core),
                )
            )
        for copy in spread:
            copy.wait_send()
        return sent, swapped

    def gather(s, sent, swapped):
        swapped[0].wait_recv()
        total = own_part[s, 0] + half_recv[s, 0]
        for copy in sent:
            copy.wait_recv()
        for d in near:
            total = total + near_recv[s, d]
        for n in range(CORES):
            total = total + far_recv[s, n]
        mine = piece_at(0, core)
        merged[s, mine] = total
        here = merged.at[s, mine]
        gathered = {
            d: send(here, here, (m_ssem, m_rsem), (s, d), leaf=leaf_at(d, core)) for d in near
        }
        straight = [
            send(here, here, (o_ssem, o_rsem), (s, n), leaf=leaf_at(far, at_core))
            for n, at_core in enumerate((core, other))
        ]
        passed = {0: send(here, here, (p_ssem, p_rsem), (s, 0), leaf=partner)}
        arrived(s, mine)
        for copy in sent + list(swapped.values()):
            copy.wait_send()
        return gathered, straight, passed

    def pass_on(s, gathered, straight, passed):
        for d in near:
            gathered[d].wait_recv()
            at = merged.at[s, piece_at(nx - d, core)]
            passed[d] = send(at, at, (p_ssem, p_rsem), (s, d), leaf=partner)

    def collect(s, gathered, straight, passed):
        for d in near:
            arrived(s, piece_at(nx - d, core))
        for d in [0] + near:
            passed[d].wait_recv()
            arrived(s, piece_at(nx - d, other))
        for copy, at_core in zip(straight, (core, other)):
            copy.wait_recv()
            arrived(s, piece_at(far, at_core))
        for copy in list(gathered.values()) + straight + list(passed.values()):
            copy.wait_send()

    def iterate(k, is_first):
        spreads = []
        for s in streams:
            alpha, beta, _, spread = condense(s, k, is_first)
            spreads.append(spread)
            finish(s, k, alpha, beta, is_first)
        moves = [merge(s, k, spreads[s]) for s in streams]
        moves = [gather(s, *moves[s]) for s in streams]
        pass_on(0, *moves[0])
        collect(0, *moves[0])
        project(0, lambda: pass_on(1, *moves[1]))
        collect(1, *moves[1])
        project(1)
        return 0

    project_first()
    iterate(0, True)
    lax.fori_loop(1, ITERS - 1, lambda k, _: iterate(k, False), 0)

    end = ITERS - 1
    ends = [condense(s, end, False) for s in streams]

    def both_streams(values):
        return select(*(both_sides(value) for value in values))

    own = both_streams([own for _, _, own, _ in ends]).sum(axis=0, keepdims=True)
    q_send[0:1, :] = own
    over_chip = send(
        q_send.at[0:1], q_recv.at[0:1], (q_ssem, q_rsem), 0, leaf=partner
    )
    totals = []
    for s, (alpha, beta, _, _) in enumerate(ends):
        advance(s, alpha, beta)
        q = jnp.zeros((8, cols), F32)
        for i in range(0, rows // 2, tile):
            new = direction[s, i : i + tile, :]
            q = q + (diag_full[i : i + tile, :] * new * new).reshape(-1, 8, cols).sum(axis=0)
        totals.append(q)
    q = both_streams(totals).sum(axis=0, keepdims=True) * (1.0 / nx)
    over_chip.wait_recv()
    q = q + (own + q_recv[0:1, :])
    g_send[0:1, :] = q
    place = x * fronts + front
    g_recv[place, 0:1, :] = q
    over_all = [
        send(
            g_send.at[0:1],
            g_recv.at[place, 0:1],
            (g_ssem, g_rsem),
            (dx * nz + dz) * ny + dy,
            leaf=leaf_at(dx, core),
            front=front_at(dz, dy),
        )
        for dx, dz, dy in chips
    ]
    for s, (alpha, _, _, _) in enumerate(ends):
        subtract(s, end - 1, alpha)

    def widen(n, _):
        at = pl.ds(pl.multiple_of(n * half_piece, half_piece), half_piece)
        to = pl.ds(pl.multiple_of(n * piece, piece), piece)
        x_out[to, :] = full(x_ref[0, at, :], x_ref[1, at, :])
        direction_out[to, :] = full(direction[0, at, :], direction[1, at, :])
        return 0

    lax.fori_loop(0, rows // piece, widen, 0)

    def widen_interior(n, _):
        at = pl.ds(pl.multiple_of(n * half_rank, half_rank), half_rank)
        to = pl.ds(pl.multiple_of(n * rank, rank), rank)
        interior_out[to, :] = full(interior[0, at, :], interior[1, at, :])
        return 0

    lax.fori_loop(0, fronts, widen_interior, 0)
    for s, (_, _, _, spread) in enumerate(ends):
        for dz, dy in peers:
            projection(s, dz, dy).wait_send()
        for copy in spread:
            copy.wait_recv()
    for n in range(fronts):
        at = slice(n * half_rank, (n + 1) * half_rank)
        last_out[n * rank : (n + 1) * rank, :] = full(c_full[end, 0, at, :], c_full[end, 1, at, :])
    for copy in over_all:
        copy.wait_recv()
    q = g_recv[0, 0:1, :]
    for n in range(1, nx * fronts):
        q = q + g_recv[n, 0:1, :]
    step_ref[...] = select(rr_ref[0], rr_ref[1]) / q
    for _, _, _, spread in ends:
        for copy in spread:
            copy.wait_send()
    for copy in [over_chip] + over_all:
        copy.wait_send()


def per_device(sources, order, diagonal, coupling, interior_inverse, interior_load, grid=(NZ, NY, NX)):
    nz, ny, nx = grid
    fronts, leaves = nz * ny, nx * CORES
    rows, cols = sources.shape
    depth = coupling.shape[1]
    blocks, rank = interior_inverse.shape[:2]
    assert blocks == fronts and depth == blocks * rank
    piece = rows // 2 // nx
    vmem = pl.BlockSpec(memory_space=pltpu.VMEM)
    dma = pltpu.SemaphoreType.DMA
    field = pltpu.VMEM((rows, cols), F32)
    halves = pltpu.VMEM((STREAMS, rows // 2, cols), F32)
    hbm = pl.BlockSpec(memory_space=pltpu.HBM)
    whole = jax.ShapeDtypeStruct((rows, cols), F32)
    inner = jax.ShapeDtypeStruct((depth, cols), F32)
    x, direction, interior, coeff, step = pl.pallas_call(
        functools.partial(front_solve, grid),
        out_shape=(whole, whole, inner, inner, jax.ShapeDtypeStruct((1, cols), F32)),
        in_specs=[hbm] * 6,
        out_specs=(vmem,) * 5,
        scratch_shapes=[
            pltpu.SMEM((rows,), jnp.int32),
            field,
            pltpu.VMEM((rows // 128, 128), F32),
            pltpu.VMEM(interior_inverse.shape, F32),
            pltpu.VMEM(interior_load.shape, F32),
            pltpu.VMEM((rows, depth), F32),
            pltpu.VMEM((rows, depth), BF16),
            pltpu.VMEM((rows, depth), BF16),
            pltpu.VMEM((depth, rows), BF16),
            pltpu.VMEM((depth, rows), BF16),
            pltpu.VMEM((STREAMS, max(rows, depth), cols), BF16),
            pltpu.VMEM((2 * cols, rows), BF16),
            field,
            halves,
            halves,
            halves,
            halves,
            pltpu.VMEM((STREAMS, depth // 2, cols), F32),
            pltpu.VMEM((rows // 2, cols), F32),
            pltpu.VMEM((STREAMS, fronts, rank // 2 + EXTRA, cols), F32),
            pltpu.VMEM((STREAMS, fronts, rank // 2 + EXTRA, cols), F32),
            pltpu.VMEM((STREAMS, rank // 2, cols), F32),
            pltpu.VMEM((ITERS, STREAMS, depth // 2, cols), F32),
            pltpu.VMEM((STREAMS, nx, piece // 2, cols), F32),
            pltpu.VMEM((STREAMS, nx, piece // 2, cols), F32),
            pltpu.VMEM((STREAMS, CORES, piece // 2, cols), F32),
            pltpu.VMEM((STREAMS, CORES, piece // 2, cols), F32),
            pltpu.VMEM((STREAMS, nx, piece // 2, cols), F32),
            pltpu.VMEM((STREAMS, nx, piece // 2, cols), F32),
            pltpu.VMEM((STREAMS, nx, piece // 2, cols), F32),
            pltpu.VMEM((STREAMS, CORES * nx, piece // 2, cols), F32),
            pltpu.VMEM((STREAMS, CORES * nx, SUMS, 8, cols), F32),
            pltpu.VMEM((STREAMS, rank // 2, cols), F32),
            pltpu.VMEM((STREAMS, rank // 2, cols), F32),
            pltpu.VMEM((STREAMS, 1, cols), F32),
            pltpu.VMEM((8, cols), F32),
            pltpu.VMEM((8, cols), F32),
            pltpu.VMEM((8, cols), F32),
            pltpu.VMEM((nx * fronts, 8, cols), F32),
            dma((5,)),
            dma((min(8, rows // 128),)),
            dma((STREAMS, fronts)),
            dma((STREAMS, fronts)),
            dma((STREAMS, fronts)),
            dma((STREAMS, fronts)),
            dma((STREAMS, nx)),
            dma((STREAMS, nx)),
            dma((STREAMS, CORES)),
            dma((STREAMS, CORES)),
            dma((STREAMS, nx)),
            dma((STREAMS, nx)),
            dma((STREAMS, nx)),
            dma((STREAMS, nx)),
            dma((STREAMS, CORES)),
            dma((STREAMS, CORES)),
            dma((STREAMS, nx)),
            dma((STREAMS, nx)),
            dma((1,)),
            dma((1,)),
            dma((nx * fronts,)),
            dma((nx * fronts,)),
        ],
        compiler_params=pltpu.CompilerParams(
            collective_id=0, has_side_effects=True, vmem_limit_bytes=48 << 20
        ),
        name="front_solve",
    )(
        *(
            pltpu.with_memory_space_constraint(value, pltpu.HBM)
            for value in (
                order,
                sources,
                diagonal.reshape(rows // 128, 128),
                coupling,
                interior_inverse,
                interior_load,
            )
        )
    )
    interior = interior - step * coeff
    return x + step * direction, interior.reshape(interior_load.shape)


def solution(mesh):
    in_specs = (
        P(("wave", "front"), None),
        P("front"),
        P(("wave", "front")),
        P(("wave", "front"), "leaf"),
        P(("wave", "leaf"), None, None),
        P(("wave", "leaf"), None, None),
    )
    out_specs = (P(("wave", "front"), None), P(("wave", "leaf"), None, None))
    return jax.shard_map(
        per_device, mesh=mesh, in_specs=in_specs, out_specs=out_specs, check_vma=False
    )
```
